256 devices in a mesh: seq: 64 (over y, z, core), layer: 4 (over x).
Axes of the slice: x: 4, y: 4, z: 8, core: 2. Of those that a mesh axis runs over, the one named last changes fastest.
Arguments:
- gradients: bfloat16 [16384, 4096], P('seq', 'layer'), may hold values from -6 to 6
- projection: bfloat16 [4096, 8192], P('layer', 'seq'), may hold values from -0.09375 to 0.09375
- queries: bfloat16 [256, 8192], P(None, 'seq'), may hold values from -6 to 6
Outputs:
- scores: float32 [16384, 256], P(('seq', 'layer'))
The draws below stay inside these ranges and needn't reach their ends.
All inputs are finite; a program needn't handle non-finite values.
Results may differ from the reference program's by a relative error of at most 0.0029.
Values may be sent and summed in bfloat16 or wider, within the bound.
A program may use at most 128 MiB of HBM per device.

```python
import math
import jax
import jax.numpy as jnp
from jax import lax

FEAT = 4096
K = 8192
Q = 256
S = 16384


def level_of(own_key, extent, split, low, high):
    gain = 1.0
    for position, blocks in split:
        steps = jax.random.uniform(jax.random.fold_in(jax.random.fold_in(own_key, 6), position), (blocks,), jnp.float32, low / len(split), high / len(split))
        gain = gain * jnp.repeat(jnp.exp(steps), extent[position] // blocks).reshape((-1,) + (1,) * (len(extent) - 1 - position))
    return gain


def centred(key, extent, spread, bound, shards=(), held_as=jnp.bfloat16):
    factor_of = level_of(key, extent, shards, -0.22, 0.18) if shards else 1.0
    array = jax.random.normal(key, extent, jnp.float32) * spread * factor_of
    return jnp.minimum(jnp.maximum(array, -bound), bound).astype(held_as)


def setup_inputs(seed: int = 0) -> dict:
    keys = jax.random.split(jax.random.key(seed), 4)
    gradients = centred(keys[0], (S, FEAT), 1.0, 6.0, ((0, 64), (1, 4)))
    projection = centred(keys[1], (FEAT, K), FEAT ** -0.5, 0.09375, ((0, 4), (1, 64)))
    queries = centred(keys[2], (Q, K), 1.0, 6.0, ((1, 64),))
    return dict(gradients=gradients, projection=projection, queries=queries)


epsilon = 1e-06

def reference(gradients, projection, queries):
    sketch = jnp.dot(gradients, projection, preferred_element_type=jnp.float32).astype(jnp.bfloat16)
    sketch_wide = sketch.astype(jnp.float32)
    row_squares = lax.optimization_barrier(jnp.sum(sketch_wide * sketch_wide, axis=1))
    query_wide = queries.astype(jnp.float32)
    query_squares = lax.optimization_barrier(jnp.sum(query_wide * query_wide, axis=1))
    products = lax.dot_general(sketch, queries, (((1,), (1,)), ((), ())), preferred_element_type=jnp.float32)
    return math.sqrt(K) * products * lax.rsqrt(row_squares + epsilon)[:, None] * lax.rsqrt(query_squares + epsilon)[None, :]
```

```python
import functools
import heapq
import math

import jax
import jax.numpy as jnp
from jax import lax
from jax.experimental import pallas as pl
from jax.experimental.pallas import tpu as pltpu
from jax.sharding import PartitionSpec as P

MESH = pl.DeviceIdType.MESH
K = 8192
EPS = 1e-06
YS, ZS, XS = 4, 8, 4
ROWS_A = 448


def halves(first, last):
    mid = (first + last) // 2
    return {0: (first, last), 1: (first, mid), 2: (mid, last)}


def step(pos, by, size):
    return (pos + by) % size


def forwards(key):
    part, oy, oz, half = key
    out = []
    zs = [("z+", (part, oy, 7, 0)), ("z-", (part, oy, 1, 0))]
    ys = [("y+", (part, 3, oz, 0)), ("y-", (part, 1, oz, 0))]
    on_y = {3: [("y+", (part, 2, oz, 1))], 1: [("y-", (part, 2, oz, 2))]}
    on_z = {
        7: [("z+", (part, oy, 6, 0))],
        6: [("z+", (part, oy, 5, 0))],
        5: [("z+", (part, oy, 4, 1))],
        1: [("z-", (part, oy, 2, 0))],
        2: [("z-", (part, oy, 3, 0))],
        3: [("z-", (part, oy, 4, 2))],
    }
    if part == "A":
        if oz == 0:
            out += ys if oy == 0 else on_y.get(oy, [])
            out += zs
        else:
            out += on_z.get(oz, [])
    else:
        if oy == 0:
            out += zs if oz == 0 else on_z.get(oz, [])
            out += ys
        else:
            out += on_y.get(oy, [])
    return out


def plan(bytes_a, bytes_b):
    rate, lag, quad_us, gather_us = 44e3, 1.8, 0.45, 20.0
    free = dict.fromkeys(["y+", "y-", "z+", "z-"], 0.0)
    size = {"A": bytes_a, "B": bytes_b}
    arrivals, order, actions = [], 0, []
    seen, whole, mine, theirs = set(), set(), {}, {}
    quads = []
    now = 0.0

    def complete(key):
        nonlocal order
        part, oy, oz, half = key
        sent = []
        for link, new in forwards(key):
            start = max(now, free[link])
            free[link] = start + size[part] / (2 if new[3] else 1) / rate
            heapq.heappush(arrivals, (free[link] + lag, order, new))
            order += 1
            sent.append((link, new))
        actions.append(("send", key[:3], sent))
        seen.add(key[:3])
        if ("A", oy, oz) in seen and ("B", oy, oz) in seen:
            actions.append(("share", oy, oz))
            mine[oz] = mine.get(oz, 0) + 1
            if mine[oz] == YS:
                quads.append((now, oz, 0))
                quads.append((now + 2.0, oz, 1))

    complete(("A", 0, 0, 0))
    complete(("B", 0, 0, 0))
    got = {}
    gathered = False
    while arrivals or quads or not gathered:
        if not gathered and now >= gather_us:
            actions.append(("gradients",))
            gathered = True
        if arrivals and arrivals[0][0] <= now:
            _, _, key = heapq.heappop(arrivals)
            actions.append(("wait", key))
            now += 0.08
            part, oy, oz, half = key
            if half:
                got[key[:3]] = got.get(key[:3], 0) + 1
                if got[key[:3]] == 2:
                    complete(key)
            else:
                complete(key)
            continue
        ready = sorted(q for q in quads if q[0] <= now)
        if gathered and ready:
            quads.remove(ready[0])
            actions.append(("quad", ready[0][1], ready[0][2]))
            now += quad_us
            continue
        nexts = [a[0] for a in arrivals[:1]] + ([min(quads)[0]] if quads and gathered else [])
        if not gathered:
            nexts.append(gather_us)
        now = max(now + 1e-6, min(nexts))
    return actions, now


def kernel(actions, spans, ids, g_hbm, p_hbm, q_hbm, out_ref, gall, pin, qin, buf, acc, fsend, frecv,
           local, gs, gr, ts, tr, ms, mr, ds, dr, fs, fr):
    s, a = lax.axis_index("seq"), lax.axis_index("layer")
    core, z, y = s % 2, (s // 2) % ZS, s // (2 * ZS)
    feats, width = p_hbm.shape
    part_rows = q_hbm.shape[0] // XS
    mine = 2 * (z % 2) + core
    swap_s = s - mine + a
    partner = s + 1 - 2 * core

    def at(yy, zz):
        return (yy * ZS + zz) * 2 + core

    ahead = {
        "y+": (at((y + 1) % YS, z), a),
        "y-": (at((y + YS - 1) % YS, z), a),
        "z+": (at(y, (z + 1) % ZS), a),
        "z-": (at(y, (z + ZS - 1) % ZS), a),
        "x+": (s, (a + 1) % XS),
        "x-": (s, (a + XS - 1) % XS),
        "x2": (s, (a + 2) % XS),
    }
    ypos = [(y + k) % YS for k in range(YS)]
    zpos = [(z + k) % ZS for k in range(ZS)]

    def remote(src, dst, send, recv, to):
        return pltpu.make_async_remote_copy(
            src_ref=src, dst_ref=dst, send_sem=send, recv_sem=recv, device_id=to, device_id_type=MESH
        )

    p_in = pltpu.make_async_copy(p_hbm, pin, local.at[0])
    q_in = pltpu.make_async_copy(q_hbm, qin, local.at[1])
    g_in = pltpu.make_async_copy(g_hbm, gall.at[a], local.at[2])
    p_in.start()
    q_in.start()
    g_in.start()

    barrier = pltpu.get_barrier_semaphore()
    around = [*ahead.values(), (partner, a)]
    for device in around:
        pl.semaphore_signal(barrier, inc=1, device_id=device, device_id_type=MESH)

    @pl.when(a != mine)
    def _():
        pl.semaphore_signal(barrier, inc=1, device_id=(swap_s, mine), device_id_type=MESH)

    @pl.when(a != mine)
    def _():
        pl.semaphore_wait(barrier, len(around) + 1)

    @pl.when(a == mine)
    def _():
        pl.semaphore_wait(barrier, len(around))

    q_rows = qin.at[pl.ds(pl.multiple_of(a * part_rows, part_rows), part_rows)]
    p_swap = remote(pin, buf.at[swap_s, pl.ds(0, feats)], ts.at[0], tr.at[0], (swap_s, mine))
    q_swap = remote(q_rows, buf.at[swap_s, pl.ds(feats, part_rows)], ts.at[1], tr.at[1], (swap_s, mine))
    p_stay = pltpu.make_async_copy(pin, buf.at[s, pl.ds(0, feats)], local.at[3])
    q_stay = pltpu.make_async_copy(q_rows, buf.at[s, pl.ds(feats, part_rows)], local.at[4])
    p_in.wait()
    q_in.wait()

    @pl.when(a != mine)
    def _():
        p_swap.start()
        q_swap.start()

    @pl.when(a == mine)
    def _():
        p_stay.start()
        q_stay.start()

    left, right, far = (a + XS - 1) % XS, (a + 1) % XS, (a + 2) % XS
    half = gall.shape[1] // 2
    g_sends = [
        remote(gall.at[a], gall.at[a], gs.at[0], gr.at[0], ahead["x+"]),
        remote(gall.at[a], gall.at[a], gs.at[1], gr.at[1], ahead["x-"]),
        remote(gall.at[left, pl.ds(0, half)], gall.at[left, pl.ds(0, half)], gs.at[2], gr.at[2], ahead["x+"]),
        remote(gall.at[right, pl.ds(half, half)], gall.at[right, pl.ds(half, half)], gs.at[3], gr.at[3], ahead["x-"]),
    ]
    g_waits = [
        remote(gall.at[left], gall.at[left], gs.at[0], gr.at[0], ahead["x+"]),
        remote(gall.at[right], gall.at[right], gs.at[1], gr.at[1], ahead["x-"]),
        remote(gall.at[far, pl.ds(0, half)], gall.at[far, pl.ds(0, half)], gs.at[2], gr.at[2], ahead["x+"]),
        remote(gall.at[far, pl.ds(half, half)], gall.at[far, pl.ds(half, half)], gs.at[3], gr.at[3], ahead["x-"]),
    ]
    g_in.wait()
    g_sends[0].start()
    g_sends[1].start()

    @pl.when(a != mine)
    def _():
        remote(pin, buf.at[s, pl.ds(0, feats)], ts.at[0], tr.at[0], (swap_s, mine)).wait_recv()
        remote(q_rows, buf.at[s, pl.ds(feats, part_rows)], ts.at[1], tr.at[1], (swap_s, mine)).wait_recv()

    @pl.when(a == mine)
    def _():
        p_stay.wait()
        q_stay.wait()

    def block(key):
        part, oy, oz, which = key
        first, last = spans[part][which]
        return buf.at[at(ypos[oy], zpos[oz]), pl.ds(first, last - first)]

    def message(link, key, view):
        return remote(view, view, ms.at[ids[key]], mr.at[ids[key]], ahead[link])

    def shared(oy, oz, whose):
        view = buf.at[whose + ((ypos[oy] * ZS + zpos[oz]) * 2)]
        return remote(view, view, ds.at[oy * ZS + oz], dr.at[oy * ZS + oz], (partner, a))

    for oz in range(acc.shape[0]):
        acc[oz] = jnp.zeros(acc.shape[1:], jnp.float32)

    def quad(zz, whose):
        layer = 2 * (zz % 2) + whose
        for pair in range(2):
            right_side = jnp.concatenate(
                [buf[(yy * ZS + zz) * 2 + whose, pl.ds(0, feats), :] for yy in (2 * pair, 2 * pair + 1)], axis=1
            )
            columns = pl.ds(pair * 2 * width, 2 * width)
            acc[zz // 2, :, columns] += jnp.dot(gall[layer], right_side, preferred_element_type=jnp.float32)

    used = {}
    for action in actions:
        if action[0] == "send":
            for link, new in action[2]:
                source = (*action[1], new[3])
                used[new] = link
                message(link, new, block(source)).start()
        elif action[0] == "share":
            shared(action[1], action[2], core).start()
        elif action[0] == "wait":
            key = action[1]
            message(used[key], key, block(key)).wait_recv()
        elif action[0] == "gradients":
            g_waits[0].wait_recv()
            g_sends[2].start()
            g_waits[1].wait_recv()
            g_sends[3].start()
            g_waits[2].wait_recv()
            g_waits[3].wait_recv()
        elif action[0] == "quad":
            oz, other = action[1:]
            if other:
                for oy in range(YS):
                    shared(oy, oz, 1 - core).wait_recv()
                quad(zpos[oz], 1 - core)
            else:
                quad(zpos[oz], core)

    rows = gall.shape[1]
    queries = q_hbm.shape[0]
    products = jnp.zeros((rows, queries), jnp.float32)
    row_squares = jnp.zeros((rows, width), jnp.float32)
    query_squares = jnp.zeros((queries, width), jnp.float32)

    def finish(group, carry):
        products, row_squares, query_squares = carry
        sketch = acc[group].astype(jnp.bfloat16)
        wide = sketch.astype(jnp.float32)
        asked = jnp.concatenate(
            [
                jnp.concatenate(
                    [buf[yy * 2 * ZS + group * 4 + layer, pl.ds(feats, part_rows), :] for layer in range(XS)], axis=0
                )
                for yy in range(YS)
            ],
            axis=1,
        )
        asked_wide = asked.astype(jnp.float32)
        for yy in range(YS):
            own = wide[:, yy * width : (yy + 1) * width]
            row_squares += own * own
            ask = asked_wide[:, yy * width : (yy + 1) * width]
            query_squares += ask * ask
        products += lax.dot_general(
            sketch, asked, (((1,), (1,)), ((), ())), preferred_element_type=jnp.float32
        )
        return products, row_squares, query_squares

    products, row_squares, query_squares = lax.fori_loop(
        0, acc.shape[0], finish, (products, row_squares, query_squares)
    )
    ones = jnp.ones((8, width), jnp.float32)

    def along(squares):
        return lax.dot_general(
            ones, squares, (((1,), (1,)), ((), ())), precision=lax.Precision.HIGHEST,
            preferred_element_type=jnp.float32,
        )

    block_rows = rows // XS
    row_line, query_line = along(row_squares), along(query_squares)
    for target in range(XS):
        fsend[target, pl.ds(0, block_rows)] = products[target * block_rows : (target + 1) * block_rows]
        fsend[target, pl.ds(block_rows, 8)] = row_line
        fsend[target, pl.ds(block_rows + 8, 8)] = query_line
    finals = []
    for k, link in ((1, "x+"), (3, "x-"), (2, "x2")):
        target = (a + k) % XS
        finals.append(remote(fsend.at[target], frecv.at[k - 1], fs.at[k - 1], fr.at[k - 1], ahead[link]))
    for copy in finals:
        copy.start()
    total = fsend[a]
    for copy in finals:
        copy.wait_recv()
    total = total + frecv[0] + frecv[1] + frecv[2]
    at_row = lax.broadcasted_iota(jnp.int32, (block_rows, rows), 0) + a * block_rows
    chosen = (lax.broadcasted_iota(jnp.int32, (block_rows, rows), 1) == at_row).astype(jnp.float32)
    own_rows = lax.dot_general(
        chosen, total[block_rows : block_rows + 8], (((1,), (1,)), ((), ())), precision=lax.Precision.HIGHEST,
        preferred_element_type=jnp.float32,
    )[:, 0:1]
    asked_squares = total[block_rows + 8 : block_rows + 9]
    out_ref[...] = (
        math.sqrt(K) * total[:block_rows] * lax.rsqrt(own_rows + EPS) * lax.rsqrt(asked_squares + EPS)
    )

    for copy in finals:
        copy.wait_send()
    for copy in g_sends:
        copy.wait_send()

    @pl.when(a != mine)
    def _():
        p_swap.wait_send()
        q_swap.wait_send()

    groups = {}
    for key in ids:
        groups.setdefault((key[0], bool(key[3])), []).append(key)
    for keys in groups.values():
        first, view = ids[keys[0]], block(keys[0])

        def sent(k, carry, view=view):
            remote(view, view, ms.at[k], mr.at[k], (partner, a)).wait_send()
            return carry

        lax.fori_loop(first, first + len(keys), sent, 0)

    def given(k, carry):
        remote(buf.at[s], buf.at[s], ds.at[k], dr.at[k], (partner, a)).wait_send()
        return carry

    lax.fori_loop(0, YS * ZS, given, 0)


def shards(gradients, projection, queries):
    rows, feats = gradients.shape
    width = projection.shape[1]
    count = queries.shape[0]
    part_rows = count // XS
    deep = feats + part_rows
    spans = {"A": halves(0, ROWS_A), "B": halves(ROWS_A, deep)}
    actions, _ = plan(ROWS_A * width * 2, (deep - ROWS_A) * width * 2)
    keys = sorted((action[1] for action in actions if action[0] == "wait"), key=lambda k: (k[0], k[3] > 0, k))
    ids = {key: k for k, key in enumerate(keys)}
    dma = pltpu.SemaphoreType.DMA
    return pl.pallas_call(
        functools.partial(kernel, actions, spans, ids),
        out_shape=jax.ShapeDtypeStruct((rows // XS, count), jnp.float32),
        in_specs=[pl.BlockSpec(memory_space=pl.ANY)] * 3,
        out_specs=pl.BlockSpec(memory_space=pltpu.VMEM),
        scratch_shapes=[
            pltpu.VMEM((XS, rows, feats), jnp.bfloat16),
            pltpu.VMEM((feats, width), jnp.bfloat16),
            pltpu.VMEM((count, width), jnp.bfloat16),
            pltpu.VMEM((2 * YS * ZS, deep, width), jnp.bfloat16),
            pltpu.VMEM((ZS // 2, rows, YS * width), jnp.float32),
            pltpu.VMEM((XS, rows // XS + 16, count), jnp.float32),
            pltpu.VMEM((XS - 1, rows // XS + 16, count), jnp.float32),
            dma((5,)), dma((4,)), dma((4,)), dma((2,)), dma((2,)),
            dma((len(keys),)), dma((len(keys),)), dma((YS * ZS,)), dma((YS * ZS,)), dma((3,)), dma((3,)),
        ],
        compiler_params=pltpu.CompilerParams(
            collective_id=0, has_side_effects=True, vmem_limit_bytes=56 * 2**20
        ),
    )(gradients, projection, queries)


def solution(mesh):
    placed = (P("seq", "layer"), P("layer", "seq"), P(None, "seq"))
    return jax.shard_map(
        shards, mesh=mesh, in_specs=placed, out_specs=P(("seq", "layer"), None), check_vma=False
    )
```

```python
import functools
import heapq
import math

import jax
import jax.numpy as jnp
from jax import lax
from jax.experimental import pallas as pl
from jax.experimental.pallas import tpu as pltpu
from jax.sharding import PartitionSpec as P

MESH = pl.DeviceIdType.MESH
K = 8192
EPS = 1e-06
YS, ZS, XS = 4, 8, 4
ROWS_A = 448


def halves(first, last):
    mid = (first + last) // 2
    return {0: (first, last), 1: (first, mid), 2: (mid, last)}


def step(pos, by, size):
    return (pos + by) % size


def forwards(key):
    part, oy, oz, half = key
    out = []
    zs = [("z+", (part, oy, 7, 0)), ("z-", (part, oy, 1, 0))]
    ys = [("y+", (part, 3, oz, 0)), ("y-", (part, 1, oz, 0))]
    on_y = {3: [("y+", (part, 2, oz, 1))], 1: [("y-", (part, 2, oz, 2))]}
    on_z = {
        7: [("z+", (part, oy, 6, 0))],
        6: [("z+", (part, oy, 5, 0))],
        5: [("z+", (part, oy, 4, 1))],
        1: [("z-", (part, oy, 2, 0))],
        2: [("z-", (part, oy, 3, 0))],
        3: [("z-", (part, oy, 4, 2))],
    }
    if part == "A":
        if oz == 0:
            out += ys if oy == 0 else on_y.get(oy, [])
            out += zs
        else:
            out += on_z.get(oz, [])
    else:
        if oy == 0:
            out += zs if oz == 0 else on_z.get(oz, [])
            out += ys
        else:
            out += on_y.get(oy, [])
    return out


def plan(bytes_a, bytes_b):
    rate, lag, quad_us, gather_us = 44e3, 1.8, 0.45, 20.0
    free = dict.fromkeys(["y+", "y-", "z+", "z-"], 0.0)
    size = {"A": bytes_a, "B": bytes_b}
    arrivals, order, actions = [], 0, []
    seen, whole, mine, theirs = set(), set(), {}, {}
    quads = []
    now = 0.0

    def complete(key):
        nonlocal order
        part, oy, oz, half = key
        sent = []
        for link, new in forwards(key):
            start = max(now, free[link])
            free[link] = start + size[part] / (2 if new[3] else 1) / rate
            heapq.heappush(arrivals, (free[link] + lag, order, new))
            order += 1
            sent.append((link, new))
        actions.append(("send", key[:3], sent))
        seen.add(key[:3])
        if ("A", oy, oz) in seen and ("B", oy, oz) in seen:
            actions.append(("share", oy, oz))
            mine[oz] = mine.get(oz, 0) + 1
            if mine[oz] == YS:
                quads.append((now, oz, 0))
                quads.append((now + 2.0, oz, 1))

    for part in ("A", "B"):
        actions.append(("own", part))
        complete((part, 0, 0, 0))
        now += 2.0
    got = {}
    gathered = False
    early = False
    while arrivals or quads or not gathered:
        if not early and len(mine) == ZS and all(n == YS for oz, n in mine.items() if oz != 4) and not any(
            q[1] != 4 for q in quads
        ):
            for oz in (0, 2, 6):
                actions.append(("finish", oz))
            now += 1.2
            early = True
        if not gathered and now >= gather_us:
            actions.append(("gradients",))
            gathered = True
        if arrivals and arrivals[0][0] <= now:
            _, _, key = heapq.heappop(arrivals)
            actions.append(("wait", key))
            now += 0.08
            part, oy, oz, half = key
            if half:
                got[key[:3]] = got.get(key[:3], 0) + 1
                if got[key[:3]] == 2:
                    complete(key)
            else:
                complete(key)
            continue
        ready = sorted(q for q in quads if q[0] <= now)
        if gathered and ready:
            quads.remove(ready[0])
            actions.append(("quad", ready[0][1], ready[0][2]))
            now += quad_us
            continue
        nexts = [a[0] for a in arrivals[:1]] + ([min(quads)[0]] if quads and gathered else [])
        if not gathered:
            nexts.append(gather_us)
        now = max(now + 1e-6, min(nexts))
    actions.append(("finish", 4))
    return actions, now


def kernel(actions, spans, ids, g_hbm, p_hbm, q_hbm, out_ref, gall, pin, qin, buf, acc, prods, rsq, qsq,
           fsend, frecv, lines, local, gs, gr, ts, tr, ms, mr, ds, dr, fs, fr):
    s, a = lax.axis_index("seq"), lax.axis_index("layer")
    core, z, y = s % 2, (s // 2) % ZS, s // (2 * ZS)
    feats, width = p_hbm.shape
    part_rows = q_hbm.shape[0] // XS
    mine = z % 2 + 2 * core
    swap_s = s - 2 * (z % 2) - core + 2 * (a % 2) + a // 2
    partner = s + 1 - 2 * core

    def at(yy, zz):
        return (yy * ZS + zz) * 2 + core

    ahead = {
        "y+": (at((y + 1) % YS, z), a),
        "y-": (at((y + YS - 1) % YS, z), a),
        "z+": (at(y, (z + 1) % ZS), a),
        "z-": (at(y, (z + ZS - 1) % ZS), a),
        "x+": (s, (a + 1) % XS),
        "x-": (s, (a + XS - 1) % XS),
        "x2": (s, (a + 2) % XS),
    }
    ypos = [(y + k) % YS for k in range(YS)]
    zpos = [(z + k) % ZS for k in range(ZS)]

    def remote(src, dst, send, recv, to):
        return pltpu.make_async_remote_copy(
            src_ref=src, dst_ref=dst, send_sem=send, recv_sem=recv, device_id=to, device_id_type=MESH
        )

    p_in = pltpu.make_async_copy(p_hbm, pin, local.at[0])
    q_in = pltpu.make_async_copy(q_hbm, qin, local.at[1])
    g_in = pltpu.make_async_copy(g_hbm, gall.at[a], local.at[2])
    p_in.start()
    q_in.start()
    g_in.start()

    barrier = pltpu.get_barrier_semaphore()
    around = [*ahead.values(), (partner, a)]
    for device in around:
        pl.semaphore_signal(barrier, inc=1, device_id=device, device_id_type=MESH)

    @pl.when(a != mine)
    def _():
        pl.semaphore_signal(barrier, inc=1, device_id=(swap_s, mine), device_id_type=MESH)

    @pl.when(a != mine)
    def _():
        pl.semaphore_wait(barrier, len(around) + 1)

    @pl.when(a == mine)
    def _():
        pl.semaphore_wait(barrier, len(around))

    q_rows = qin.at[pl.ds(pl.multiple_of(a * part_rows, part_rows), part_rows)]
    cuts = [(0, ROWS_A), (ROWS_A, feats), (feats, feats + part_rows)]

    def swap(k, place):
        first, last = cuts[k]
        view = q_rows if k == 2 else pin.at[pl.ds(first, last - first)]
        return remote(view, buf.at[place, pl.ds(first, last - first)], ts.at[k], tr.at[k], (swap_s, mine))

    def stay(k):
        first, last = cuts[k]
        view = q_rows if k == 2 else pin.at[pl.ds(first, last - first)]
        return pltpu.make_async_copy(view, buf.at[s, pl.ds(first, last - first)], local.at[3 + k])

    p_in.wait()
    q_in.wait()

    @pl.when(a != mine)
    def _():
        for k in range(3):
            swap(k, swap_s).start()

    @pl.when(a == mine)
    def _():
        for k in range(3):
            stay(k).start()

    left, right, far = (a + XS - 1) % XS, (a + 1) % XS, (a + 2) % XS
    half = gall.shape[1] // 2
    g_sends = [
        remote(gall.at[a], gall.at[a], gs.at[0], gr.at[0], ahead["x+"]),
        remote(gall.at[a], gall.at[a], gs.at[1], gr.at[1], ahead["x-"]),
        remote(gall.at[left, pl.ds(0, half)], gall.at[left, pl.ds(0, half)], gs.at[2], gr.at[2], ahead["x+"]),
        remote(gall.at[right, pl.ds(half, half)], gall.at[right, pl.ds(half, half)], gs.at[3], gr.at[3], ahead["x-"]),
    ]
    g_waits = [
        remote(gall.at[left], gall.at[left], gs.at[0], gr.at[0], ahead["x+"]),
        remote(gall.at[right], gall.at[right], gs.at[1], gr.at[1], ahead["x-"]),
        remote(gall.at[far, pl.ds(0, half)], gall.at[far, pl.ds(0, half)], gs.at[2], gr.at[2], ahead["x+"]),
        remote(gall.at[far, pl.ds(half, half)], gall.at[far, pl.ds(half, half)], gs.at[3], gr.at[3], ahead["x-"]),
    ]
    g_in.wait()
    g_sends[0].start()
    g_sends[1].start()

    def arrived(parts):
        @pl.when(a != mine)
        def _():
            for k in parts:
                swap(k, s).wait_recv()

        @pl.when(a == mine)
        def _():
            for k in parts:
                stay(k).wait()

    def block(key):
        part, oy, oz, which = key
        first, last = spans[part][which]
        return buf.at[at(ypos[oy], zpos[oz]), pl.ds(first, last - first)]

    def message(link, key, view):
        return remote(view, view, ms.at[ids[key]], mr.at[ids[key]], ahead[link])

    def shared(oy, oz, whose):
        view = buf.at[whose + ((ypos[oy] * ZS + zpos[oz]) * 2)]
        return remote(view, view, ds.at[oy * ZS + oz], dr.at[oy * ZS + oz], (partner, a))

    for oz in range(acc.shape[0]):
        acc[oz] = jnp.zeros(acc.shape[1:], jnp.float32)

    def quad(zz, whose):
        layer = zz % 2 + 2 * whose
        for pair in range(2):
            right_side = jnp.concatenate(
                [buf[(yy * ZS + zz) * 2 + whose, pl.ds(0, feats), :] for yy in (2 * pair, 2 * pair + 1)], axis=1
            )
            columns = pl.ds(pair * 2 * width, 2 * width)
            acc[zz // 2, :, columns] += jnp.dot(gall[layer], right_side, preferred_element_type=jnp.float32)

    rows = gall.shape[1]
    prods[...] = jnp.zeros(prods.shape, jnp.float32)
    rsq[...] = jnp.zeros(rsq.shape, jnp.float32)
    qsq[...] = jnp.zeros(qsq.shape, jnp.float32)

    def finish(group):
        sketch = acc[group].astype(jnp.bfloat16)
        wide = sketch.astype(jnp.float32)
        asked = jnp.concatenate(
            [
                jnp.concatenate(
                    [
                        buf[yy * 2 * ZS + group * 4 + 2 * (layer % 2) + layer // 2, pl.ds(feats, part_rows), :]
                        for layer in range(XS)
                    ],
                    axis=0,
                )
                for yy in range(YS)
            ],
            axis=1,
        )
        asked_wide = asked.astype(jnp.float32)
        row_part, query_part = rsq[...], qsq[...]
        for yy in range(YS):
            own = wide[:, yy * width : (yy + 1) * width]
            row_part += own * own
            ask = asked_wide[:, yy * width : (yy + 1) * width]
            query_part += ask * ask
        rsq[...], qsq[...] = row_part, query_part
        prods[...] += lax.dot_general(
            sketch, asked, (((1,), (1,)), ((), ())), preferred_element_type=jnp.float32
        )

    used = {}
    for action in actions:
        if action[0] == "own":
            arrived((0,) if action[1] == "A" else (1, 2))
        elif action[0] == "send":
            for link, new in action[2]:
                source = (*action[1], new[3])
                used[new] = link
                message(link, new, block(source)).start()
        elif action[0] == "share":
            shared(action[1], action[2], core).start()
        elif action[0] == "wait":
            key = action[1]
            message(used[key], key, block(key)).wait_recv()
        elif action[0] == "gradients":
            g_waits[0].wait_recv()
            g_sends[2].start()
            g_waits[1].wait_recv()
            g_sends[3].start()
            g_waits[2].wait_recv()
            g_waits[3].wait_recv()
        elif action[0] == "finish":
            finish(zpos[action[1]] // 2)
        elif action[0] == "quad":
            oz, other = action[1:]
            if other:
                for oy in range(YS):
                    shared(oy, oz, 1 - core).wait_recv()
                quad(zpos[oz], 1 - core)
            else:
                quad(zpos[oz], core)

    ones = jnp.ones((8, width), jnp.float32)

    def along(squares):
        return lax.dot_general(
            ones, squares, (((1,), (1,)), ((), ())), precision=lax.Precision.HIGHEST,
            preferred_element_type=jnp.float32,
        )

    block_rows = rows // XS
    lines[0, pl.ds(0, 8)] = along(rsq[...])
    lines[0, pl.ds(8, 8)] = along(qsq[...])
    for target in range(XS):
        fsend[target] = prods[target * block_rows : (target + 1) * block_rows].astype(jnp.bfloat16)
    finals = []
    for k, link in ((2, "x2"), (1, "x+"), (3, "x-")):
        target = (a + k) % XS
        finals.append(remote(fsend.at[target], frecv.at[k - 1], fs.at[k - 1], fr.at[k - 1], ahead[link]))
        finals.append(remote(lines.at[0], lines.at[k], fs.at[k + 2], fr.at[k + 2], ahead[link]))
    for copy in finals:
        copy.start()
    total = prods[pl.ds(pl.multiple_of(a * block_rows, block_rows), block_rows)]
    for copy in finals:
        copy.wait_recv()
    for k in range(XS - 1):
        total = total + frecv[k].astype(jnp.float32)
    line = lines[0] + lines[1] + lines[2] + lines[3]
    at_row = lax.broadcasted_iota(jnp.int32, (block_rows, rows), 0) + a * block_rows
    chosen = (lax.broadcasted_iota(jnp.int32, (block_rows, rows), 1) == at_row).astype(jnp.float32)
    own_rows = lax.dot_general(
        chosen, line[0:8], (((1,), (1,)), ((), ())), precision=lax.Precision.HIGHEST,
        preferred_element_type=jnp.float32,
    )[:, 0:1]
    asked_squares = line[8:9]
    out_ref[...] = (
        math.sqrt(K) * total * lax.rsqrt(own_rows + EPS) * lax.rsqrt(asked_squares + EPS)
    )

    for copy in finals:
        copy.wait_send()
    for copy in g_sends:
        copy.wait_send()

    @pl.when(a != mine)
    def _():
        for k in range(3):
            swap(k, swap_s).wait_send()

    groups = {}
    for key in ids:
        groups.setdefault((key[0], bool(key[3])), []).append(key)
    for keys in groups.values():
        first, view = ids[keys[0]], block(keys[0])

        def sent(k, carry, view=view):
            remote(view, view, ms.at[k], mr.at[k], (partner, a)).wait_send()
            return carry

        lax.fori_loop(first, first + len(keys), sent, 0)

    def given(k, carry):
        remote(buf.at[s], buf.at[s], ds.at[k], dr.at[k], (partner, a)).wait_send()
        return carry

    lax.fori_loop(0, YS * ZS, given, 0)


def shards(gradients, projection, queries):
    rows, feats = gradients.shape
    width = projection.shape[1]
    count = queries.shape[0]
    part_rows = count // XS
    deep = feats + part_rows
    spans = {"A": halves(0, ROWS_A), "B": halves(ROWS_A, deep)}
    actions, _ = plan(ROWS_A * width * 2, (deep - ROWS_A) * width * 2)
    keys = sorted((action[1] for action in actions if action[0] == "wait"), key=lambda k: (k[0], k[3] > 0, k))
    ids = {key: k for k, key in enumerate(keys)}
    dma = pltpu.SemaphoreType.DMA
    return pl.pallas_call(
        functools.partial(kernel, actions, spans, ids),
        out_shape=jax.ShapeDtypeStruct((rows // XS, count), jnp.float32),
        in_specs=[pl.BlockSpec(memory_space=pl.ANY)] * 3,
        out_specs=pl.BlockSpec(memory_space=pltpu.VMEM),
        scratch_shapes=[
            pltpu.VMEM((XS, rows, feats), jnp.bfloat16),
            pltpu.VMEM((feats, width), jnp.bfloat16),
            pltpu.VMEM((count, width), jnp.bfloat16),
            pltpu.VMEM((2 * YS * ZS, deep, width), jnp.bfloat16),
            pltpu.VMEM((ZS // 2, rows, YS * width), jnp.float32),
            pltpu.VMEM((rows, count), jnp.float32),
            pltpu.VMEM((rows, width), jnp.float32),
            pltpu.VMEM((count, width), jnp.float32),
            pltpu.VMEM((XS, rows // XS, count), jnp.bfloat16),
            pltpu.VMEM((XS - 1, rows // XS, count), jnp.bfloat16),
            pltpu.VMEM((XS, 16, count), jnp.float32),
            dma((6,)), dma((4,)), dma((4,)), dma((3,)), dma((3,)),
            dma((len(keys),)), dma((len(keys),)), dma((YS * ZS,)), dma((YS * ZS,)), dma((6,)), dma((6,)),
        ],
        compiler_params=pltpu.CompilerParams(
            collective_id=0, has_side_effects=True, vmem_limit_bytes=56 * 2**20
        ),
    )(gradients, projection, queries)


def solution(mesh):
    placed = (P("seq", "layer"), P("layer", "seq"), P(None, "seq"))
    return jax.shard_map(
        shards, mesh=mesh, in_specs=placed, out_specs=P(("seq", "layer"), None), check_vma=False
    )
```

```python
import functools
import heapq
import math

import jax
import jax.numpy as jnp
from jax import lax
from jax.experimental import pallas as pl
from jax.experimental.pallas import tpu as pltpu
from jax.sharding import PartitionSpec as P

MESH = pl.DeviceIdType.MESH
K = 8192
EPS = 1e-06
YS, ZS, XS = 4, 8, 4
PARTS = (("B", 352), ("B", 320), ("A", 416))


def spans_of(parts):
    spans, first = [], 0
    for _, rows in parts:
        mid, last = first + rows // 2, first + rows
        spans.append({0: (first, last), 1: (first, mid), 2: (mid, last)})
        first = last
    return spans


def forwards(key):
    part, oy, oz, half = key
    out = []
    zs = [("z+", (part, oy, 7, 0)), ("z-", (part, oy, 1, 0))]
    ys = [("y+", (part, 3, oz, 0)), ("y-", (part, 1, oz, 0))]
    on_y = {3: [("y+", (part, 2, oz, 1))], 1: [("y-", (part, 2, oz, 2))]}
    on_z = {
        7: [("z+", (part, oy, 6, 0))],
        6: [("z+", (part, oy, 5, 0))],
        5: [("z+", (part, oy, 4, 1))],
        1: [("z-", (part, oy, 2, 0))],
        2: [("z-", (part, oy, 3, 0))],
        3: [("z-", (part, oy, 4, 2))],
    }
    if PARTS[part][0] == "A":
        if oz == 0:
            out += ys if oy == 0 else on_y.get(oy, [])
            out += zs
        else:
            out += on_z.get(oz, [])
    else:
        if oy == 0:
            out += zs if oz == 0 else on_z.get(oz, [])
            out += ys
        else:
            out += on_y.get(oy, [])
    return out


def plan(row_bytes):
    rate, lag, unit_us, event_us = 46.6e3, 1.9, 0.08, 0.08
    gathers = [20.0, 30.0]
    free = dict.fromkeys(["y+", "y-", "z+", "z-"], 0.0)
    arrivals, order, actions = [], 0, []
    seen, mine, got = set(), {}, {}
    units = []
    now = 0.0

    def complete(key):
        nonlocal order
        part, oy, oz, half = key
        sent = []
        for link, new in forwards(key):
            start = max(now, free[link])
            free[link] = start + PARTS[part][1] * row_bytes / (2 if new[3] else 1) / rate
            heapq.heappush(arrivals, (free[link] + lag, order, new))
            order += 1
            sent.append((link, new))
        actions.append(("send", key[:3], sent))
        seen.add(key[:3])
        if all((p, oy, oz) in seen for p in range(len(PARTS))):
            actions.append(("share", oy, oz))
            mine[oz] = mine.get(oz, 0) + 1
            if mine[oz] == YS:
                units.extend((now, oz, 0, k) for k in range(4))
                units.extend((now + 2.0, oz, 1, k) for k in range(4))

    at = 4.0
    for part, (_, rows) in enumerate(PARTS):
        at += rows * row_bytes / rate
        heapq.heappush(arrivals, (at, order, (part, 0, 0, 0)))
        order += 1
    gathered, early = 0, False

    def compute():
        nonlocal now
        ready = sorted(u for u in units if u[0] <= now)
        if gathered < 2 or not ready:
            return False
        units.remove(ready[0])
        actions.append(("unit", *ready[0][1:]))
        now += unit_us
        return True

    while arrivals or units or gathered < 2:
        if gathered < 2 and now >= gathers[gathered]:
            actions.append(("gradients", gathered))
            gathered += 1
        if not early and sum(mine.get(oz, 0) for oz in range(ZS) if oz != 4) == YS * (ZS - 1) and all(
            u[1] == 4 for u in units
        ):
            for oz in (0, 2, 6):
                actions.append(("finish", oz))
                now += 0.1
            early = True
        if arrivals and arrivals[0][0] <= now:
            _, _, key = heapq.heappop(arrivals)
            actions.append(("wait", key) if any(key[1:3]) else ("own", key[0]))
            now += event_us
            if key[3]:
                got[key[:3]] = got.get(key[:3], 0) + 1
                if got[key[:3]] == 2:
                    complete(key)
            else:
                complete(key)
            compute()
            continue
        if (not arrivals or arrivals[0][0] > now + 1.5 * unit_us) and compute():
            continue
        nexts = [a[0] for a in arrivals[:1]] + ([min(units)[0]] if units and gathered == 2 else [])
        if gathered < 2:
            nexts.append(gathers[gathered])
        now = max(now + 1e-6, min(nexts))
    actions.append(("finish", 4))
    return actions, now


def kernel(actions, spans, ids, g_hbm, p_hbm, q_hbm, out_ref, gall, pin, qin, buf, acc, prods, rsq, qsq,
           fsend, frecv, lines, local, gs, gr, ts, tr, ms, mr, ds, dr, fs, fr):
    s, a = lax.axis_index("seq"), lax.axis_index("layer")
    core, z, y = s % 2, (s // 2) % ZS, s // (2 * ZS)
    feats, width = p_hbm.shape
    part_rows = q_hbm.shape[0] // XS
    mine = z % 2 + 2 * core
    swap_s = s - 2 * (z % 2) - core + 2 * (a % 2) + a // 2
    partner = s + 1 - 2 * core

    def at(yy, zz):
        return (yy * ZS + zz) * 2 + core

    ahead = {
        "y+": (at((y + 1) % YS, z), a),
        "y-": (at((y + YS - 1) % YS, z), a),
        "z+": (at(y, (z + 1) % ZS), a),
        "z-": (at(y, (z + ZS - 1) % ZS), a),
        "x+": (s, (a + 1) % XS),
        "x-": (s, (a + XS - 1) % XS),
        "x2": (s, (a + 2) % XS),
    }
    ypos = [(y + k) % YS for k in range(YS)]
    zpos = [(z + k) % ZS for k in range(ZS)]

    def remote(src, dst, send, recv, to):
        return pltpu.make_async_remote_copy(
            src_ref=src, dst_ref=dst, send_sem=send, recv_sem=recv, device_id=to, device_id_type=MESH
        )

    p_in = pltpu.make_async_copy(p_hbm, pin, local.at[0])
    q_in = pltpu.make_async_copy(q_hbm, qin, local.at[1])
    g_in = pltpu.make_async_copy(g_hbm, gall.at[a], local.at[2])
    p_in.start()
    q_in.start()
    g_in.start()

    barrier = pltpu.get_barrier_semaphore()
    around = [*ahead.values(), (partner, a)]
    for device in around:
        pl.semaphore_signal(barrier, inc=1, device_id=device, device_id_type=MESH)

    @pl.when(a != mine)
    def _():
        pl.semaphore_signal(barrier, inc=1, device_id=(swap_s, mine), device_id_type=MESH)

    @pl.when(a != mine)
    def _():
        pl.semaphore_wait(barrier, len(around) + 1)

    @pl.when(a == mine)
    def _():
        pl.semaphore_wait(barrier, len(around))

    q_rows = qin.at[pl.ds(pl.multiple_of(a * part_rows, part_rows), part_rows)]
    cuts = [span[0] for span in spans]
    last_part = len(cuts) - 1
    cuts = [*cuts[:-1], (cuts[-1][0], feats), (feats, feats + part_rows)]

    def swap(k, place):
        first, last = cuts[k]
        view = q_rows if k > last_part else pin.at[pl.ds(first, last - first)]
        return remote(view, buf.at[place, pl.ds(first, last - first)], ts.at[k], tr.at[k], (swap_s, mine))

    def stay(k):
        first, last = cuts[k]
        view = q_rows if k > last_part else pin.at[pl.ds(first, last - first)]
        return pltpu.make_async_copy(view, buf.at[s, pl.ds(first, last - first)], local.at[3 + k])

    p_in.wait()
    q_in.wait()

    @pl.when(a != mine)
    def _():
        for k in range(len(cuts)):
            swap(k, swap_s).start()

    @pl.when(a == mine)
    def _():
        for k in range(len(cuts)):
            stay(k).start()

    left, right, far = (a + XS - 1) % XS, (a + 1) % XS, (a + 2) % XS
    half = gall.shape[1] // 2
    g_sends = [
        remote(gall.at[a], gall.at[a], gs.at[0], gr.at[0], ahead["x+"]),
        remote(gall.at[a], gall.at[a], gs.at[1], gr.at[1], ahead["x-"]),
        remote(gall.at[left, pl.ds(0, half)], gall.at[left, pl.ds(0, half)], gs.at[2], gr.at[2], ahead["x+"]),
        remote(gall.at[right, pl.ds(half, half)], gall.at[right, pl.ds(half, half)], gs.at[3], gr.at[3], ahead["x-"]),
    ]
    g_waits = [
        remote(gall.at[left], gall.at[left], gs.at[0], gr.at[0], ahead["x+"]),
        remote(gall.at[right], gall.at[right], gs.at[1], gr.at[1], ahead["x-"]),
        remote(gall.at[far, pl.ds(0, half)], gall.at[far, pl.ds(0, half)], gs.at[2], gr.at[2], ahead["x+"]),
        remote(gall.at[far, pl.ds(half, half)], gall.at[far, pl.ds(half, half)], gs.at[3], gr.at[3], ahead["x-"]),
    ]
    g_in.wait()
    g_sends[0].start()
    g_sends[1].start()

    def arrived(parts):
        @pl.when(a != mine)
        def _():
            for k in parts:
                swap(k, s).wait_recv()

        @pl.when(a == mine)
        def _():
            for k in parts:
                stay(k).wait()

    def block(key):
        part, oy, oz, which = key
        first, last = spans[part][which]
        return buf.at[at(ypos[oy], zpos[oz]), pl.ds(first, last - first)]

    def message(link, key, view):
        return remote(view, view, ms.at[ids[key]], mr.at[ids[key]], ahead[link])

    def shared(oy, oz, whose):
        view = buf.at[whose + ((ypos[oy] * ZS + zpos[oz]) * 2)]
        return remote(view, view, ds.at[oy * ZS + oz], dr.at[oy * ZS + oz], (partner, a))

    for oz in range(acc.shape[0]):
        acc[oz] = jnp.zeros(acc.shape[1:], jnp.float32)

    def unit(zz, whose, k):
        layer, pair = zz % 2 + 2 * whose, k // 2
        deep = pl.ds(k % 2 * (feats // 2), feats // 2)
        right_side = jnp.concatenate(
            [buf[(yy * ZS + zz) * 2 + whose, deep, :] for yy in (2 * pair, 2 * pair + 1)], axis=1
        )
        columns = pl.ds(pair * 2 * width, 2 * width)
        acc[zz // 2, :, columns] += jnp.dot(gall[layer, :, deep], right_side, preferred_element_type=jnp.float32)

    rows = gall.shape[1]
    prods[...] = jnp.zeros(prods.shape, jnp.float32)
    rsq[...] = jnp.zeros(rsq.shape, jnp.float32)
    qsq[...] = jnp.zeros(qsq.shape, jnp.float32)

    def finish(group):
        sketch = acc[group].astype(jnp.bfloat16)
        wide = sketch.astype(jnp.float32)
        asked = jnp.concatenate(
            [
                jnp.concatenate(
                    [
                        buf[yy * 2 * ZS + group * 4 + 2 * (layer % 2) + layer // 2, pl.ds(feats, part_rows), :]
                        for layer in range(XS)
                    ],
                    axis=0,
                )
                for yy in range(YS)
            ],
            axis=1,
        )
        asked_wide = asked.astype(jnp.float32)
        row_part, query_part = rsq[...], qsq[...]
        for yy in range(YS):
            own = wide[:, yy * width : (yy + 1) * width]
            row_part += own * own
            ask = asked_wide[:, yy * width : (yy + 1) * width]
            query_part += ask * ask
        rsq[...], qsq[...] = row_part, query_part
        prods[...] += lax.dot_general(
            sketch, asked, (((1,), (1,)), ((), ())), preferred_element_type=jnp.float32
        )

    used = {}
    for action in actions:
        if action[0] == "own":
            arrived((action[1],) if action[1] < last_part else (last_part, last_part + 1))
        elif action[0] == "send":
            for link, new in action[2]:
                source = (*action[1], new[3])
                used[new] = link
                message(link, new, block(source)).start()
        elif action[0] == "share":
            shared(action[1], action[2], core).start()
        elif action[0] == "wait":
            key = action[1]
            message(used[key], key, block(key)).wait_recv()
        elif action[0] == "gradients":
            for k in (0, 1) if action[1] == 0 else (2, 3):
                g_waits[k].wait_recv()
                if k < 2:
                    g_sends[k + 2].start()
        elif action[0] == "finish":
            finish(zpos[action[1]] // 2)
        elif action[0] == "unit":
            oz, other, k = action[1:]
            if other and k == 0:
                for oy in range(YS):
                    shared(oy, oz, 1 - core).wait_recv()
            unit(zpos[oz], 1 - core if other else core, k)

    ones = jnp.ones((8, width), jnp.float32)

    def along(squares):
        return lax.dot_general(
            ones, squares, (((1,), (1,)), ((), ())), precision=lax.Precision.HIGHEST,
            preferred_element_type=jnp.float32,
        )

    block_rows = rows // XS
    lines[0, pl.ds(0, 8)] = along(rsq[...])
    lines[0, pl.ds(8, 8)] = along(qsq[...])
    for target in range(XS):
        fsend[target] = prods[target * block_rows : (target + 1) * block_rows].astype(jnp.bfloat16)
    finals = []
    for k, link in ((2, "x2"), (1, "x+"), (3, "x-")):
        target = (a + k) % XS
        finals.append(remote(fsend.at[target], frecv.at[k - 1], fs.at[k - 1], fr.at[k - 1], ahead[link]))
        finals.append(remote(lines.at[0], lines.at[k], fs.at[k + 2], fr.at[k + 2], ahead[link]))
    for copy in finals:
        copy.start()
    total = prods[pl.ds(pl.multiple_of(a * block_rows, block_rows), block_rows)]
    for copy in finals:
        copy.wait_recv()
    for k in range(XS - 1):
        total = total + frecv[k].astype(jnp.float32)
    line = lines[0] + lines[1] + lines[2] + lines[3]
    at_row = lax.broadcasted_iota(jnp.int32, (block_rows, rows), 0) + a * block_rows
    chosen = (lax.broadcasted_iota(jnp.int32, (block_rows, rows), 1) == at_row).astype(jnp.float32)
    own_rows = lax.dot_general(
        chosen, line[0:8], (((1,), (1,)), ((), ())), precision=lax.Precision.HIGHEST,
        preferred_element_type=jnp.float32,
    )[:, 0:1]
    asked_squares = line[8:9]
    out_ref[...] = (
        math.sqrt(K) * total * lax.rsqrt(own_rows + EPS) * lax.rsqrt(asked_squares + EPS)
    )

    for copy in finals:
        copy.wait_send()
    for copy in g_sends:
        copy.wait_send()

    @pl.when(a != mine)
    def _():
        for k in range(len(cuts)):
            swap(k, swap_s).wait_send()

    groups = {}
    for key in ids:
        groups.setdefault((key[0], bool(key[3])), []).append(key)
    for keys in groups.values():
        first, view = ids[keys[0]], block(keys[0])

        def sent(k, carry, view=view):
            remote(view, view, ms.at[k], mr.at[k], (partner, a)).wait_send()
            return carry

        lax.fori_loop(first, first + len(keys), sent, 0)

    def given(k, carry):
        remote(buf.at[s], buf.at[s], ds.at[k], dr.at[k], (partner, a)).wait_send()
        return carry

    lax.fori_loop(0, YS * ZS, given, 0)


def shards(gradients, projection, queries):
    rows, feats = gradients.shape
    width = projection.shape[1]
    count = queries.shape[0]
    part_rows = count // XS
    deep = feats + part_rows
    assert sum(part[1] for part in PARTS) == deep
    spans = spans_of(PARTS)
    actions, _ = plan(width * 2)
    keys = sorted((action[1] for action in actions if action[0] == "wait"), key=lambda k: (k[0], k[3] > 0, k))
    ids = {key: k for k, key in enumerate(keys)}
    dma = pltpu.SemaphoreType.DMA
    return pl.pallas_call(
        functools.partial(kernel, actions, spans, ids),
        out_shape=jax.ShapeDtypeStruct((rows // XS, count), jnp.float32),
        in_specs=[pl.BlockSpec(memory_space=pl.ANY)] * 3,
        out_specs=pl.BlockSpec(memory_space=pltpu.VMEM),
        scratch_shapes=[
            pltpu.VMEM((XS, rows, feats), jnp.bfloat16),
            pltpu.VMEM((feats, width), jnp.bfloat16),
            pltpu.VMEM((count, width), jnp.bfloat16),
            pltpu.VMEM((2 * YS * ZS, deep, width), jnp.bfloat16),
            pltpu.VMEM((ZS // 2, rows, YS * width), jnp.float32),
            pltpu.VMEM((rows, count), jnp.float32),
            pltpu.VMEM((rows, width), jnp.float32),
            pltpu.VMEM((count, width), jnp.float32),
            pltpu.VMEM((XS, rows // XS, count), jnp.bfloat16),
            pltpu.VMEM((XS - 1, rows // XS, count), jnp.bfloat16),
            pltpu.VMEM((XS, 16, count), jnp.float32),
            dma((4 + len(PARTS),)), dma((4,)), dma((4,)), dma((1 + len(PARTS),)), dma((1 + len(PARTS),)),
            dma((len(keys),)), dma((len(keys),)), dma((YS * ZS,)), dma((YS * ZS,)), dma((6,)), dma((6,)),
        ],
        compiler_params=pltpu.CompilerParams(
            collective_id=0, has_side_effects=True, vmem_limit_bytes=56 * 2**20
        ),
    )(gradients, projection, queries)


def solution(mesh):
    placed = (P("seq", "layer"), P("layer", "seq"), P(None, "seq"))
    return jax.shard_map(
        shards, mesh=mesh, in_specs=placed, out_specs=P(("seq", "layer"), None), check_vma=False
    )
```

```python
import functools
import heapq
import math

import jax
import jax.numpy as jnp
from jax import lax
from jax.experimental import pallas as pl
from jax.experimental.pallas import tpu as pltpu
from jax.sharding import PartitionSpec as P

MESH = pl.DeviceIdType.MESH
K = 8192
EPS = 1e-06
XS, YS, ZS = 4, 4, 8
RING = ZS // 2
PARTS = (("B", 480), ("B", 480), ("A", 128))


def spans_of(parts):
    spans, first = [], 0
    for _, rows in parts:
        mid, last = first + rows // 2, first + rows
        spans.append({0: (first, last), 1: (first, mid), 2: (mid, last)})
        first = last
    return spans


def forwards(key):
    part, oy, oz, half = key
    own_y = [("y+", (part, 3, oz, 0)), ("y-", (part, 1, oz, 0))]
    own_z = [("z+", (part, oy, 3, 0)), ("z-", (part, oy, 1, 0))]
    on_y = {0: own_y, 3: [("y+", (part, 2, oz, 1))], 1: [("y-", (part, 2, oz, 2))], 2: []}
    on_z = {0: own_z, 3: [("z+", (part, oy, 2, 1))], 1: [("z-", (part, oy, 2, 2))], 2: []}
    if PARTS[part][0] == "A":
        return on_y[oy] + own_z if oz == 0 else on_z[oz]
    return on_z[oz] + own_y if oy == 0 else on_y[oy]


def plan(row_bytes, piece_bytes):
    lag, unit_us, event_us, start_us = 1.9, 0.08, 0.08, 4.0
    rate = {"y+": 46.6e3, "y-": 46.6e3, "z+": 23.3e3, "z-": 23.3e3, "x+": 46.6e3, "x-": 46.6e3}
    free = dict.fromkeys(rate, 0.0)
    free["x+"] = free["x-"] = 6.0
    arrivals, order, actions = [], 0, []
    seen, mine, got, pieces = set(), {}, {}, {0: 0, 1: 0}
    units = []
    now = 0.0

    def send(link, key, size):
        nonlocal order
        begin = max(now, free[link])
        free[link] = begin + size / rate[link]
        heapq.heappush(arrivals, (free[link] + lag, order, key))
        order += 1

    def at_time(when, key):
        nonlocal order
        heapq.heappush(arrivals, (when, order, key))
        order += 1

    def complete(key):
        part, oy, oz, half = key
        sent = forwards(key)
        for link, new in sent:
            send(link, new, PARTS[part][1] * row_bytes / (2 if new[3] else 1))
        actions.append(("send", key[:3], sent))
        seen.add(key[:3])
        if all((p, oy, oz) in seen for p in range(len(PARTS))):
            actions.append(("share", oy, oz))
            whole = (oy % 2, oz)
            mine[whole] = mine.get(whole, 0) + 1
            if mine[whole] == 2:
                for group in range(2):
                    units.extend((now, oy % 2, oz, 0, group, k) for k in range(2))
                    units.extend((now + 2.0, oy % 2, oz, 1, group, k) for k in range(2))

    def offer(group, h):
        send("x+", ("G", group, 3, h), piece_bytes)
        send("x-", ("G", group, 1, h), piece_bytes)

    at = start_us
    for part, (_, rows) in enumerate(PARTS):
        at += rows * row_bytes / 46.6e3
        at_time(at, (part, 0, 0, 0))
    offer(0, 0)
    offer(0, 1)
    at_time(10.0, ("W", 0))
    at_time(20.0, ("W", 1))
    done = {(oz, group): 0 for oz in range(RING) for group in range(2)}

    def compute():
        nonlocal now
        ready = sorted(u for u in units if u[0] <= now and pieces[u[4]] == 6)
        if not ready:
            return False
        pick = ready[0]
        units.remove(pick)
        actions.append(("unit", *pick[1:]))
        now += unit_us
        done[pick[2], pick[4]] += 1
        if done[pick[2], pick[4]] == 8:
            actions.append(("finish", pick[2], pick[4]))
            now += unit_us
        return True

    while arrivals or units:
        if arrivals and arrivals[0][0] <= now:
            _, _, key = heapq.heappop(arrivals)
            now += event_us
            if key[0] == "W":
                actions.append(("swapped", key[1]))
                offer(1, key[1])
            elif key[0] == "G":
                actions.append(("gradients", *key[1:]))
                pieces[key[1]] += 1
                if key[2:] == (3, 0):
                    send("x+", ("G", key[1], 2, 0), piece_bytes)
                elif key[2:] == (1, 1):
                    send("x-", ("G", key[1], 2, 1), piece_bytes)
            else:
                actions.append(("wait", key) if any(key[1:3]) else ("own", key[0]))
                if key[3]:
                    got[key[:3]] = got.get(key[:3], 0) + 1
                    if got[key[:3]] == 2:
                        complete(key)
                else:
                    complete(key)
            compute()
            continue
        if (not arrivals or arrivals[0][0] > now + 1.5 * unit_us) and compute():
            continue
        nexts = [a[0] for a in arrivals[:1]] + [u[0] for u in units if pieces[u[4]] == 6]
        now = max(now + 1e-6, min(nexts))
    return actions, now


def kernel(actions, spans, ids, g_hbm, p_hbm, q_hbm, out_ref, gall, pin, qin, buf, acc, prods, rsq, qsq,
           fsend, frecv, lsend, lrecv, local, ws, wr, gs, gr, ts, tr, ms, mr, ds, dr, fs, fr):
    s, a = lax.axis_index("seq"), lax.axis_index("layer")
    core, z, y = s % 2, (s // 2) % ZS, s // (2 * ZS)
    feats, width = p_hbm.shape
    rows, queries = g_hbm.shape[0], q_hbm.shape[0]
    part_rows = queries // XS
    mine = y % 2 + 2 * core
    group = z % 2
    partner = s + 1 - 2 * core

    def seq(yy, zz, cc):
        return (yy * ZS + zz) * 2 + cc

    def slot(yy, jj, cc):
        return (yy * RING + jj) * 2 + cc

    swap_y, swap_core = y - y % 2 + a % 2, a // 2
    swap_to = (seq(swap_y, z, swap_core), mine)
    across = z + 1 - 2 * group
    ahead = {
        "y+": (seq((y + 1) % YS, z, core), a),
        "y-": (seq((y + YS - 1) % YS, z, core), a),
        "z+": (seq(y, (z + 2) % ZS, core), a),
        "z-": (seq(y, (z + ZS - 2) % ZS, core), a),
        "x+": (s, (a + 1) % XS),
        "x-": (s, (a + XS - 1) % XS),
    }
    targets = [(3 + k, 1, (a + k) % XS, (seq(y, across, core), (a + k) % XS)) for k in (2, 1, 3, 0)]
    targets += [(k - 1, 0, (a + k) % XS, (s, (a + k) % XS)) for k in (2, 1, 3)]
    ypos = [(y + k) % YS for k in range(YS)]
    jpos = [(z // 2 + k) % RING for k in range(RING)]

    def remote(src, dst, send, recv, to):
        return pltpu.make_async_remote_copy(
            src_ref=src, dst_ref=dst, send_sem=send, recv_sem=recv, device_id=to, device_id_type=MESH
        )

    p_in = pltpu.make_async_copy(p_hbm, pin, local.at[0])
    q_in = pltpu.make_async_copy(q_hbm, qin, local.at[1])
    g_in = pltpu.make_async_copy(g_hbm, gall.at[group, a], local.at[2])
    p_in.start()
    q_in.start()
    g_in.start()

    barrier = pltpu.get_barrier_semaphore()
    around = [*ahead.values(), *(target[3] for target in targets), (partner, a)]
    del around[4:6]
    for device in around:
        pl.semaphore_signal(barrier, inc=1, device_id=device, device_id_type=MESH)

    @pl.when(a != mine)
    def _():
        pl.semaphore_signal(barrier, inc=1, device_id=swap_to, device_id_type=MESH)
        pl.semaphore_wait(barrier, len(around) + 1)

    @pl.when(a == mine)
    def _():
        pl.semaphore_wait(barrier, len(around))

    q_rows = qin.at[pl.ds(pl.multiple_of(a * part_rows, part_rows), part_rows)]
    cuts = [span[0] for span in spans]
    last_part = len(cuts) - 1
    cuts = [*cuts[:-1], (cuts[-1][0], feats), (feats, feats + part_rows)]
    here = slot(y, z // 2, core)

    def swap(k, place):
        first, last = cuts[k]
        view = q_rows if k > last_part else pin.at[pl.ds(first, last - first)]
        return remote(view, buf.at[place, pl.ds(first, last - first)], ts.at[k], tr.at[k], swap_to)

    def stay(k):
        first, last = cuts[k]
        view = q_rows if k > last_part else pin.at[pl.ds(first, last - first)]
        return pltpu.make_async_copy(view, buf.at[here, pl.ds(first, last - first)], local.at[3 + k])

    p_in.wait()
    q_in.wait()

    @pl.when(a != mine)
    def _():
        for k in range(len(cuts)):
            swap(k, slot(swap_y, z // 2, swap_core)).start()

    @pl.when(a == mine)
    def _():
        for k in range(len(cuts)):
            stay(k).start()

    def arrived(parts):
        @pl.when(a != mine)
        def _():
            for k in parts:
                swap(k, here).wait_recv()

        @pl.when(a == mine)
        def _():
            for k in parts:
                stay(k).wait()

    piece = rows // 2

    def handed(h, whose):
        view = gall.at[whose, a, pl.ds(h * piece, piece)]
        return remote(view, view, ws.at[h], wr.at[h], (seq(y, across, core), a))

    def ringed(other, came, h, layer):
        view = gall.at[1 - group if other else group, layer, pl.ds(h * piece, piece)]
        k = other * 6 + {3: 0, 1: 2, 2: 4}[came] + h
        link = {3: "x+", 1: "x-", 2: "x-" if h else "x+"}[came]
        return remote(view, view, gs.at[k], gr.at[k], ahead[link])

    left, right, far = (a + XS - 1) % XS, (a + 1) % XS, (a + 2) % XS
    g_in.wait()
    handed(0, group).start()
    for h in range(2):
        ringed(0, 3, h, a).start()
        ringed(0, 1, h, a).start()

    def block(key):
        part, oy, oz, which = key
        first, last = spans[part][which]
        return buf.at[slot(ypos[oy], jpos[oz], core), pl.ds(first, last - first)]

    def message(link, key, view):
        return remote(view, view, ms.at[ids[key]], mr.at[ids[key]], ahead[link])

    def shared(oy, oz, whose):
        view = buf.at[slot(ypos[oy], jpos[oz], whose)]
        return remote(view, view, ds.at[oy * RING + oz], dr.at[oy * RING + oz], (partner, a))

    for ref in (acc, prods, rsq, qsq):
        ref[...] = jnp.zeros(ref.shape, jnp.float32)

    def unit(parity, jj, whose, rowset, k):
        layer = parity + 2 * whose
        deep = pl.ds(k * (feats // 2), feats // 2)
        right_side = jnp.concatenate([buf[slot(parity + yy, jj, whose), deep, :] for yy in (0, 2)], axis=1)
        acc[jj, rowset] += jnp.dot(gall[rowset, layer, :, deep], right_side, preferred_element_type=jnp.float32)

    def finish(jj, rowset, other):
        sketch = acc[jj, rowset].astype(jnp.bfloat16)
        wide = sketch.astype(jnp.float32)
        asked = jnp.concatenate(
            [
                jnp.concatenate(
                    [buf[slot(layer % 2 + yy, jj, layer // 2), pl.ds(feats, part_rows), :] for layer in range(XS)],
                    axis=0,
                )
                for yy in (0, 2)
            ],
            axis=1,
        )
        own = wide * wide
        rsq[other] += own[:, :width] + own[:, width:]
        if not other:
            asked_wide = asked.astype(jnp.float32)
            ask = asked_wide * asked_wide
            qsq[...] += ask[:, :width] + ask[:, width:]
        prods[other] += lax.dot_general(
            sketch, asked, (((1,), (1,)), ((), ())), preferred_element_type=jnp.float32
        )

    used = {}
    for action in actions:
        if action[0] == "own":
            arrived((action[1],) if action[1] < last_part else (last_part, last_part + 1))
        elif action[0] == "send":
            for link, new in action[2]:
                used[new] = link
                message(link, new, block((*action[1], new[3]))).start()
            if action[1] == (0, 0, 0):
                handed(1, group).start()
        elif action[0] == "share":
            shared(action[1], action[2], core).start()
        elif action[0] == "wait":
            key = action[1]
            message(used[key], key, block(key)).wait_recv()
        elif action[0] == "swapped":
            h = action[1]
            handed(h, 1 - group).wait_recv()
            ringed(1, 3, h, a).start()
            ringed(1, 1, h, a).start()
        elif action[0] == "gradients":
            other, came, h = action[1:]
            ringed(other, came, h, {3: left, 1: right, 2: far}[came]).wait_recv()
            if (came, h) == (3, 0):
                ringed(other, 2, 0, left).start()
            elif (came, h) == (1, 1):
                ringed(other, 2, 1, right).start()
        elif action[0] == "unit":
            op, oz, their, other, k = action[1:]
            if their and not other and k == 0:
                for oy in (op, op + 2):
                    shared(oy, oz, 1 - core).wait_recv()
            unit((y + op) % 2, jpos[oz], 1 - core if their else core, 1 - group if other else group, k)
        elif action[0] == "finish":
            oz, other = action[1:]
            finish(jpos[oz], 1 - group if other else group, other)

    ones = jnp.ones((8, width), jnp.float32)

    def along(squares):
        return lax.dot_general(
            ones, squares, (((1,), (1,)), ((), ())), precision=lax.Precision.HIGHEST,
            preferred_element_type=jnp.float32,
        )

    block_rows = rows // XS
    query_line = along(qsq[...])
    for other in range(2):
        lsend[other, pl.ds(0, 8)] = along(rsq[other])
        lsend[other, pl.ds(8, 8)] = query_line
        for layer in range(XS):
            fsend[other, layer] = prods[other, layer * block_rows : (layer + 1) * block_rows].astype(jnp.bfloat16)
    finals = []
    for k, other, layer, device in targets:
        finals.append(remote(fsend.at[other, layer], frecv.at[k], fs.at[k], fr.at[k], device))
        finals.append(remote(lsend.at[other], lrecv.at[k], fs.at[7 + k], fr.at[7 + k], device))
    for copy in finals:
        copy.start()
    total = prods[0, pl.ds(pl.multiple_of(a * block_rows, block_rows), block_rows)]
    line = lsend[0]
    for copy in finals:
        copy.wait_recv()
    for k in range(7):
        total = total + frecv[k].astype(jnp.float32)
        line = line + lrecv[k]
    at_row = lax.broadcasted_iota(jnp.int32, (block_rows, rows), 0) + a * block_rows
    chosen = (lax.broadcasted_iota(jnp.int32, (block_rows, rows), 1) == at_row).astype(jnp.float32)
    own_rows = lax.dot_general(
        chosen, line[0:8], (((1,), (1,)), ((), ())), precision=lax.Precision.HIGHEST,
        preferred_element_type=jnp.float32,
    )[:, 0:1]
    out_ref[...] = math.sqrt(K) * total * lax.rsqrt(own_rows + EPS) * lax.rsqrt(line[8:9] + EPS)

    for copy in finals:
        copy.wait_send()
    for h in range(2):
        handed(h, group).wait_send()

    def rung(k, carry):
        view = gall.at[0, 0, pl.ds(0, piece)]
        remote(view, view, gs.at[k], gr.at[k], (partner, a)).wait_send()
        return carry

    lax.fori_loop(0, 12, rung, 0)

    @pl.when(a != mine)
    def _():
        for k in range(len(cuts)):
            swap(k, slot(swap_y, z // 2, swap_core)).wait_send()

    groups = {}
    for key in ids:
        groups.setdefault((key[0], bool(key[3])), []).append(key)
    for keys in groups.values():
        first, view = ids[keys[0]], block(keys[0])

        def sent(k, carry, view=view):
            remote(view, view, ms.at[k], mr.at[k], (partner, a)).wait_send()
            return carry

        lax.fori_loop(first, first + len(keys), sent, 0)

    def given(k, carry):
        remote(buf.at[0], buf.at[0], ds.at[k], dr.at[k], (partner, a)).wait_send()
        return carry

    lax.fori_loop(0, YS * RING, given, 0)


def shards(gradients, projection, queries):
    rows, feats = gradients.shape
    width = projection.shape[1]
    count = queries.shape[0]
    deep = feats + count // XS
    assert sum(part[1] for part in PARTS) == deep
    spans = spans_of(PARTS)
    actions, _ = plan(width * 2, rows * feats)
    keys = sorted((action[1] for action in actions if action[0] == "wait"), key=lambda k: (k[0], k[3] > 0, k))
    ids = {key: k for k, key in enumerate(keys)}
    dma = pltpu.SemaphoreType.DMA
    cuts = len(PARTS) + 1
    return pl.pallas_call(
        functools.partial(kernel, actions, spans, ids),
        out_shape=jax.ShapeDtypeStruct((rows // XS, count), jnp.float32),
        in_specs=[pl.BlockSpec(memory_space=pl.ANY)] * 3,
        out_specs=pl.BlockSpec(memory_space=pltpu.VMEM),
        scratch_shapes=[
            pltpu.VMEM((2, XS, rows, feats), jnp.bfloat16),
            pltpu.VMEM((feats, width), jnp.bfloat16),
            pltpu.VMEM((count, width), jnp.bfloat16),
            pltpu.VMEM((2 * YS * RING, deep, width), jnp.bfloat16),
            pltpu.VMEM((RING, 2, rows, 2 * width), jnp.float32),
            pltpu.VMEM((2, rows, count), jnp.float32),
            pltpu.VMEM((2, rows, width), jnp.float32),
            pltpu.VMEM((count, width), jnp.float32),
            pltpu.VMEM((2, XS, rows // XS, count), jnp.bfloat16),
            pltpu.VMEM((7, rows // XS, count), jnp.bfloat16),
            pltpu.VMEM((2, 16, count), jnp.float32),
            pltpu.VMEM((7, 16, count), jnp.float32),
            dma((3 + cuts,)), dma((2,)), dma((2,)), dma((12,)), dma((12,)), dma((cuts,)), dma((cuts,)),
            dma((len(keys),)), dma((len(keys),)), dma((YS * RING,)), dma((YS * RING,)), dma((14,)), dma((14,)),
        ],
        compiler_params=pltpu.CompilerParams(
            collective_id=0, has_side_effects=True, vmem_limit_bytes=56 * 2**20
        ),
    )(gradients, projection, queries)


def solution(mesh):
    placed = (P("seq", "layer"), P("layer", "seq"), P(None, "seq"))
    return jax.shard_map(
        shards, mesh=mesh, in_specs=placed, out_specs=P(("seq", "layer"), None), check_vma=False
    )
```

```python
import functools
import heapq
import math

import jax
import jax.numpy as jnp
from jax import lax
from jax.experimental import pallas as pl
from jax.experimental.pallas import tpu as pltpu
from jax.sharding import PartitionSpec as P

MESH = pl.DeviceIdType.MESH
K = 8192
EPS = 1e-06
XS, YS, ZS = 4, 4, 8
RING = ZS // 2
PARTS = (("B", 512), ("B", 576))


def spans_of(parts):
    spans, first = [], 0
    for _, rows in parts:
        mid, last = first + rows // 2, first + rows
        spans.append({0: (first, last), 1: (first, mid), 2: (mid, last)})
        first = last
    return spans


def forwards(key):
    part, oy, oz, half = key
    own_y = [("y+", (part, 3, oz, 0)), ("y-", (part, 1, oz, 0))]
    own_z = [("z+", (part, oy, 3, 0)), ("z-", (part, oy, 1, 0))]
    on_y = {0: own_y, 3: [("y+", (part, 2, oz, 1))], 1: [("y-", (part, 2, oz, 2))], 2: []}
    on_z = {0: own_z, 3: [("z+", (part, oy, 2, 1))], 1: [("z-", (part, oy, 2, 2))], 2: []}
    if PARTS[part][0] == "A":
        return on_y[oy] + own_z if oz == 0 else on_z[oz]
    return on_z[oz] + own_y if oy == 0 else on_y[oy]


def plan(row_bytes, piece_bytes):
    lag, unit_us, event_us, start_us = 3.2, 0.08, 0.08, 4.0
    rate = {"y+": 46.6e3, "y-": 46.6e3, "z+": 23.3e3, "z-": 23.3e3, "x+": 46.6e3, "x-": 46.6e3}
    free = dict.fromkeys(rate, 0.0)
    free["x+"] = free["x-"] = 6.0
    arrivals, order, actions = [], 0, []
    mine, got = {}, {}
    pieces = {(group, away): 0 for group in range(2) for away in range(XS)}
    pieces[0, 0] = 2
    units, taken = [], set()
    now = 0.0

    def send(link, key, size):
        nonlocal order
        begin = max(now, free[link])
        free[link] = begin + size / rate[link]
        heapq.heappush(arrivals, (free[link] + lag, order, key))
        order += 1

    def at_time(when, key):
        nonlocal order
        heapq.heappush(arrivals, (when, order, key))
        order += 1

    def complete(key):
        part, oy, oz, half = key
        sent = forwards(key)
        for link, new in sent:
            send(link, new, PARTS[part][1] * row_bytes / (2 if new[3] else 1))
        actions.append(("send", key[:3], sent))
        actions.append(("share", *key[:3]))
        mine[part, oz] = mine.get((part, oz), 0) + 1
        if mine[part, oz] == YS:
            units.extend((now + 2.0, oz, group, away, part) for away in (0, 1, 3, 2) for group in range(2))

    def offer(group, h):
        send("x+", ("G", group, 3, h), piece_bytes)
        send("x-", ("G", group, 1, h), piece_bytes)

    at = start_us
    for part, (_, rows) in enumerate(PARTS):
        at += rows * row_bytes / 46.6e3
        at_time(at, (part, 0, 0, 0))
    offer(0, 0)
    offer(0, 1)
    at_time(10.0, ("W", 0))
    at_time(20.0, ("W", 1))
    done = {(oz, group): 0 for oz in range(RING) for group in range(2)}

    def compute():
        nonlocal now
        ready = [u for u in units if u[0] <= now and pieces[u[2], u[3]] == 2]
        if not ready:
            return False
        pick = ready[0]
        if (pick[4], pick[1]) not in taken:
            actions.append(("take", pick[4], pick[1]))
            taken.add((pick[4], pick[1]))
        units.remove(pick)
        actions.append(("unit", *pick[1:]))
        now += unit_us
        done[pick[1:3]] += 1
        if done[pick[1:3]] == 8:
            actions.append(("finish", *pick[1:3]))
            now += unit_us
        return True

    while arrivals or units:
        if arrivals and arrivals[0][0] <= now:
            _, _, key = heapq.heappop(arrivals)
            now += event_us
            if key[0] == "W":
                actions.append(("swapped", key[1]))
                pieces[1, 0] += 1
                offer(1, key[1])
            elif key[0] == "G":
                actions.append(("gradients", *key[1:]))
                pieces[key[1:3]] += 1
                if key[2:] == (3, 0):
                    send("x+", ("G", key[1], 2, 0), piece_bytes)
                elif key[2:] == (1, 1):
                    send("x-", ("G", key[1], 2, 1), piece_bytes)
            else:
                actions.append(("wait", key) if any(key[1:3]) else ("own", key[0]))
                if key[3]:
                    got[key[:3]] = got.get(key[:3], 0) + 1
                    if got[key[:3]] == 2:
                        complete(key)
                else:
                    complete(key)
            compute()
            continue
        if (not arrivals or arrivals[0][0] > now + 1.5 * unit_us) and compute():
            continue
        nexts = [a[0] for a in arrivals[:1]] + [u[0] for u in units if pieces[u[2], u[3]] == 2]
        now = max(now + 1e-6, min(nexts))
    return actions, now


def kernel(actions, spans, ids, g_hbm, p_hbm, q_hbm, out_ref, gall, pin, qin, buf, acc, prods, rsq, qsq,
           fsend, frecv, lsend, lrecv, local, ws, wr, gs, gr, ts, tr, ms, mr, ds, dr, fs, fr):
    s, a = lax.axis_index("seq"), lax.axis_index("layer")
    core, z, y = s % 2, (s // 2) % ZS, s // (2 * ZS)
    feats, width = p_hbm.shape
    rows, queries = g_hbm.shape[0], q_hbm.shape[0]
    part_rows = queries // XS
    mine = y % 2 + 2 * core
    group = z % 2
    partner = s + 1 - 2 * core

    def seq(yy, zz, cc):
        return (yy * ZS + zz) * 2 + cc

    def slot(yy, jj, cc):
        return (yy * RING + jj) * 2 + cc

    swap_y, swap_core = y - y % 2 + a % 2, a // 2
    swap_to = (seq(swap_y, z, swap_core), mine)
    across = z + 1 - 2 * group
    ahead = {
        "y+": (seq((y + 1) % YS, z, core), a),
        "y-": (seq((y + YS - 1) % YS, z, core), a),
        "z+": (seq(y, (z + 2) % ZS, core), a),
        "z-": (seq(y, (z + ZS - 2) % ZS, core), a),
        "x+": (s, (a + 1) % XS),
        "x-": (s, (a + XS - 1) % XS),
    }
    targets = [(3 + k, 1, (a + k) % XS, (seq(y, across, core), (a + k) % XS)) for k in (2, 1, 3, 0)]
    targets += [(k - 1, 0, (a + k) % XS, (s, (a + k) % XS)) for k in (2, 1, 3)]
    ypos = [(y + k) % YS for k in range(YS)]
    jpos = [(z // 2 + k) % RING for k in range(RING)]

    def remote(src, dst, send, recv, to):
        return pltpu.make_async_remote_copy(
            src_ref=src, dst_ref=dst, send_sem=send, recv_sem=recv, device_id=to, device_id_type=MESH
        )

    p_in = pltpu.make_async_copy(p_hbm, pin, local.at[0])
    q_in = pltpu.make_async_copy(q_hbm, qin, local.at[1])
    g_in = pltpu.make_async_copy(g_hbm, gall.at[group, a], local.at[2])
    p_in.start()
    q_in.start()
    g_in.start()

    barrier = pltpu.get_barrier_semaphore()
    around = [*ahead.values(), *(target[3] for target in targets), (partner, a)]
    del around[4:6]
    for device in around:
        pl.semaphore_signal(barrier, inc=1, device_id=device, device_id_type=MESH)

    @pl.when(a != mine)
    def _():
        pl.semaphore_signal(barrier, inc=1, device_id=swap_to, device_id_type=MESH)
        pl.semaphore_wait(barrier, len(around) + 1)

    @pl.when(a == mine)
    def _():
        pl.semaphore_wait(barrier, len(around))

    q_rows = qin.at[pl.ds(pl.multiple_of(a * part_rows, part_rows), part_rows)]
    cuts = [span[0] for span in spans]
    last_part = len(cuts) - 1
    cuts = [*cuts[:-1], (cuts[-1][0], feats), (feats, feats + part_rows)]
    here = slot(y, z // 2, core)

    def swap(k, place):
        first, last = cuts[k]
        view = q_rows if k > last_part else pin.at[pl.ds(first, last - first)]
        return remote(view, buf.at[place, pl.ds(first, last - first)], ts.at[k], tr.at[k], swap_to)

    def stay(k):
        first, last = cuts[k]
        view = q_rows if k > last_part else pin.at[pl.ds(first, last - first)]
        return pltpu.make_async_copy(view, buf.at[here, pl.ds(first, last - first)], local.at[3 + k])

    p_in.wait()
    q_in.wait()

    @pl.when(a != mine)
    def _():
        for k in range(len(cuts)):
            swap(k, slot(swap_y, z // 2, swap_core)).start()

    @pl.when(a == mine)
    def _():
        for k in range(len(cuts)):
            stay(k).start()

    def arrived(parts):
        @pl.when(a != mine)
        def _():
            for k in parts:
                swap(k, here).wait_recv()

        @pl.when(a == mine)
        def _():
            for k in parts:
                stay(k).wait()

    piece = rows // 2

    def handed(h, whose):
        view = gall.at[whose, a, pl.ds(h * piece, piece)]
        return remote(view, view, ws.at[h], wr.at[h], (seq(y, across, core), a))

    def ringed(other, came, h, layer):
        view = gall.at[1 - group if other else group, layer, pl.ds(h * piece, piece)]
        k = other * 6 + {3: 0, 1: 2, 2: 4}[came] + h
        link = {3: "x+", 1: "x-", 2: "x-" if h else "x+"}[came]
        return remote(view, view, gs.at[k], gr.at[k], ahead[link])

    left, right, far = (a + XS - 1) % XS, (a + 1) % XS, (a + 2) % XS
    g_in.wait()
    handed(0, group).start()
    for h in range(2):
        ringed(0, 3, h, a).start()
        ringed(0, 1, h, a).start()

    def block(key):
        part, oy, oz, which = key
        first, last = spans[part][which]
        return buf.at[slot(ypos[oy], jpos[oz], core), pl.ds(first, last - first)]

    def message(link, key, view):
        return remote(view, view, ms.at[ids[key]], mr.at[ids[key]], ahead[link])

    def shared(part, oy, oz, whose):
        first, last = spans[part][0]
        view = buf.at[slot(ypos[oy], jpos[oz], whose), pl.ds(first, last - first)]
        k = (part * YS + oy) * RING + oz
        return remote(view, view, ds.at[k], dr.at[k], (partner, a))

    for ref in (acc, prods, rsq, qsq):
        ref[...] = jnp.zeros(ref.shape, jnp.float32)

    def unit(jj, rowset, layer, k):
        parity, whose = layer % 2, layer // 2
        deep = pl.ds(k * (feats // 2), feats // 2)
        right_side = jnp.concatenate([buf[slot(parity + yy, jj, whose), deep, :] for yy in (0, 2)], axis=1)
        acc[jj, rowset] += jnp.dot(gall[rowset, layer, :, deep], right_side, preferred_element_type=jnp.float32)

    def finish(jj, rowset, other):
        sketch = acc[jj, rowset].astype(jnp.bfloat16)
        wide = sketch.astype(jnp.float32)
        asked = jnp.concatenate(
            [
                jnp.concatenate(
                    [buf[slot(layer % 2 + yy, jj, layer // 2), pl.ds(feats, part_rows), :] for layer in range(XS)],
                    axis=0,
                )
                for yy in (0, 2)
            ],
            axis=1,
        )
        own = wide * wide
        rsq[other] += own[:, :width] + own[:, width:]
        if not other:
            asked_wide = asked.astype(jnp.float32)
            ask = asked_wide * asked_wide
            qsq[...] += ask[:, :width] + ask[:, width:]
        prods[other] += lax.dot_general(
            sketch, asked, (((1,), (1,)), ((), ())), preferred_element_type=jnp.float32
        )

    used = {}
    for action in actions:
        if action[0] == "own":
            arrived((action[1],) if action[1] < last_part else (last_part, last_part + 1))
        elif action[0] == "send":
            for link, new in action[2]:
                used[new] = link
                message(link, new, block((*action[1], new[3]))).start()
            if action[1] == (0, 0, 0):
                handed(1, group).start()
        elif action[0] == "share":
            shared(*action[1:], core).start()
        elif action[0] == "wait":
            key = action[1]
            message(used[key], key, block(key)).wait_recv()
        elif action[0] == "swapped":
            h = action[1]
            handed(h, 1 - group).wait_recv()
            ringed(1, 3, h, a).start()
            ringed(1, 1, h, a).start()
        elif action[0] == "gradients":
            other, came, h = action[1:]
            ringed(other, came, h, {3: left, 1: right, 2: far}[came]).wait_recv()
            if (came, h) == (3, 0):
                ringed(other, 2, 0, left).start()
            elif (came, h) == (1, 1):
                ringed(other, 2, 1, right).start()
        elif action[0] == "take":
            for oy in range(YS):
                shared(action[1], oy, action[2], 1 - core).wait_recv()
        elif action[0] == "unit":
            oz, other, away, k = action[1:]
            unit(jpos[oz], 1 - group if other else group, (a + away) % XS, k)
        elif action[0] == "finish":
            oz, other = action[1:]
            finish(jpos[oz], 1 - group if other else group, other)

    ones = jnp.ones((8, width), jnp.float32)

    def along(squares):
        return lax.dot_general(
            ones, squares, (((1,), (1,)), ((), ())), precision=lax.Precision.HIGHEST,
            preferred_element_type=jnp.float32,
        )

    block_rows = rows // XS
    query_line = along(qsq[...])
    upper = lax.broadcasted_iota(jnp.int32, query_line.shape, 0) < 4
    for other in range(2):
        lsend[other] = jnp.where(upper, along(rsq[other]), query_line)
        for layer in range(XS):
            fsend[other, layer] = prods[other, layer * block_rows : (layer + 1) * block_rows].astype(jnp.bfloat16)
    finals = []
    for k, other, layer, device in targets:
        finals.append(remote(fsend.at[other, layer], frecv.at[k], fs.at[k], fr.at[k], device))
        finals.append(remote(lsend.at[other], lrecv.at[k], fs.at[7 + k], fr.at[7 + k], device))
    for copy in finals:
        copy.start()
    total = prods[0, pl.ds(pl.multiple_of(a * block_rows, block_rows), block_rows)]
    line = lsend[0]
    for copy in finals:
        copy.wait_recv()
    for k in range(7):
        total = total + frecv[k].astype(jnp.float32)
        line = line + lrecv[k]
    at_row = lax.broadcasted_iota(jnp.int32, (block_rows, rows), 0) + a * block_rows
    chosen = (lax.broadcasted_iota(jnp.int32, (block_rows, rows), 1) == at_row).astype(jnp.float32)
    own_rows = lax.dot_general(
        chosen, line, (((1,), (1,)), ((), ())), precision=lax.Precision.HIGHEST,
        preferred_element_type=jnp.float32,
    )[:, 0:1]
    out_ref[...] = math.sqrt(K) * total * lax.rsqrt(own_rows + EPS) * lax.rsqrt(line[4:5] + EPS)

    for copy in finals:
        copy.wait_send()
    for h in range(2):
        handed(h, group).wait_send()

    def rung(k, carry):
        view = gall.at[0, 0, pl.ds(0, piece)]
        remote(view, view, gs.at[k], gr.at[k], (partner, a)).wait_send()
        return carry

    lax.fori_loop(0, 12, rung, 0)

    @pl.when(a != mine)
    def _():
        for k in range(len(cuts)):
            swap(k, slot(swap_y, z // 2, swap_core)).wait_send()

    groups = {}
    for key in ids:
        groups.setdefault((key[0], bool(key[3])), []).append(key)
    for keys in groups.values():
        first, view = ids[keys[0]], block(keys[0])

        def sent(k, carry, view=view):
            remote(view, view, ms.at[k], mr.at[k], (partner, a)).wait_send()
            return carry

        lax.fori_loop(first, first + len(keys), sent, 0)

    for part in range(len(spans)):
        first, last = spans[part][0]
        view = buf.at[0, pl.ds(first, last - first)]

        def given(k, carry, view=view):
            remote(view, view, ds.at[k], dr.at[k], (partner, a)).wait_send()
            return carry

        lax.fori_loop(part * YS * RING, (part + 1) * YS * RING, given, 0)


def shards(gradients, projection, queries):
    rows, feats = gradients.shape
    width = projection.shape[1]
    count = queries.shape[0]
    deep = feats + count // XS
    assert sum(part[1] for part in PARTS) == deep
    spans = spans_of(PARTS)
    actions, _ = plan(width * 2, rows * feats)
    keys = sorted((action[1] for action in actions if action[0] == "wait"), key=lambda k: (k[0], k[3] > 0, k))
    ids = {key: k for k, key in enumerate(keys)}
    dma = pltpu.SemaphoreType.DMA
    cuts = len(PARTS) + 1
    return pl.pallas_call(
        functools.partial(kernel, actions, spans, ids),
        out_shape=jax.ShapeDtypeStruct((rows // XS, count), jnp.float32),
        in_specs=[pl.BlockSpec(memory_space=pl.ANY)] * 3,
        out_specs=pl.BlockSpec(memory_space=pltpu.VMEM),
        scratch_shapes=[
            pltpu.VMEM((2, XS, rows, feats), jnp.bfloat16),
            pltpu.VMEM((feats, width), jnp.bfloat16),
            pltpu.VMEM((count, width), jnp.bfloat16),
            pltpu.VMEM((2 * YS * RING, deep, width), jnp.bfloat16),
            pltpu.VMEM((RING, 2, rows, 2 * width), jnp.float32),
            pltpu.VMEM((2, rows, count), jnp.float32),
            pltpu.VMEM((2, rows, width), jnp.float32),
            pltpu.VMEM((count, width), jnp.float32),
            pltpu.VMEM((2, XS, rows // XS, count), jnp.bfloat16),
            pltpu.VMEM((7, rows // XS, count), jnp.bfloat16),
            pltpu.VMEM((2, 8, count), jnp.float32),
            pltpu.VMEM((7, 8, count), jnp.float32),
            dma((3 + cuts,)), dma((2,)), dma((2,)), dma((12,)), dma((12,)), dma((cuts,)), dma((cuts,)),
            dma((len(keys),)), dma((len(keys),)), dma((len(PARTS) * YS * RING,)), dma((len(PARTS) * YS * RING,)), dma((14,)), dma((14,)),
        ],
        compiler_params=pltpu.CompilerParams(
            collective_id=0, has_side_effects=True, vmem_limit_bytes=56 * 2**20
        ),
    )(gradients, projection, queries)


def solution(mesh):
    placed = (P("seq", "layer"), P("layer", "seq"), P(None, "seq"))
    return jax.shard_map(
        shards, mesh=mesh, in_specs=placed, out_specs=P(("seq", "layer"), None), check_vma=False
    )
```

```python
import functools
import heapq
import math

import jax
import jax.numpy as jnp
from jax import lax
from jax.experimental import pallas as pl
from jax.experimental.pallas import tpu as pltpu
from jax.sharding import PartitionSpec as P

MESH = pl.DeviceIdType.MESH
K = 8192
EPS = 1e-06
XS, YS, ZS = 4, 4, 8
RING = ZS // 2
PARTS = (("B", 512), ("B", 576))


def spans_of(parts):
    spans, first = [], 0
    for _, rows in parts:
        mid, last = first + rows // 2, first + rows
        spans.append({0: (first, last), 1: (first, mid), 2: (mid, last)})
        first = last
    return spans


def forwards(key):
    part, oy, oz, half = key
    own_y = [("y+", (part, 3, oz, 0)), ("y-", (part, 1, oz, 0))]
    own_z = [("z+", (part, oy, 3, 0)), ("z-", (part, oy, 1, 0))]
    on_y = {0: own_y, 3: [("y+", (part, 2, oz, 1))], 1: [("y-", (part, 2, oz, 2))], 2: []}
    on_z = {0: own_z, 3: [("z+", (part, oy, 2, 1))], 1: [("z-", (part, oy, 2, 2))], 2: []}
    if PARTS[part][0] == "A":
        return on_y[oy] + own_z if oz == 0 else on_z[oz]
    return (own_y + own_z if oz == 0 else on_z[oz] + own_y) if oy == 0 else on_y[oy]


def plan(row_bytes, piece_bytes):
    lag, unit_us, event_us, start_us = 3.2, 0.08, 0.08, 4.0
    rate = {"y+": 42e3, "y-": 42e3, "z+": 21e3, "z-": 21e3, "x+": 46.6e3, "x-": 46.6e3}
    free = dict.fromkeys(rate, 0.0)
    free["x+"] = free["x-"] = 6.0
    arrivals, order, actions = [], 0, []
    mine, got = {}, {}
    pieces = {(group, away): 0 for group in range(2) for away in range(XS)}
    pieces[0, 0] = 2
    units, taken = [], set()
    now = 0.0

    def send(link, key, size):
        nonlocal order
        begin = max(now, free[link])
        free[link] = begin + size / rate[link]
        heapq.heappush(arrivals, (free[link] + lag, order, key))
        order += 1

    def at_time(when, key):
        nonlocal order
        heapq.heappush(arrivals, (when, order, key))
        order += 1

    def complete(key):
        part, oy, oz, half = key
        sent = forwards(key)
        for link, new in sent:
            send(link, new, PARTS[part][1] * row_bytes / (2 if new[3] else 1))
        actions.append(("send", key[:3], sent))
        actions.append(("share", *key[:3]))
        mine[part, oz] = mine.get((part, oz), 0) + 1
        if mine[part, oz] == YS:
            units.extend((now + 2.0, oz, group, away, part) for group in (1, 0) for away in (0, 1, 3, 2))

    def offer(group, h):
        send("x+", ("G", group, 3, h), piece_bytes)
        send("x-", ("G", group, 1, h), piece_bytes)

    at = start_us
    for part, (_, rows) in enumerate(PARTS):
        at += rows * row_bytes / 46.6e3
        at_time(at, (part, 0, 0, 0))
    offer(0, 0)
    offer(0, 1)
    at_time(10.0, ("W", 0))
    at_time(20.0, ("W", 1))
    done = {(oz, group): 0 for oz in range(RING) for group in range(2)}

    def compute():
        nonlocal now
        ready = [u for u in units if u[0] <= now and pieces[u[2], u[3]] == 2]
        if not ready:
            return False
        pick = ready[0]
        if (pick[4], pick[1]) not in taken:
            actions.append(("take", pick[4], pick[1]))
            taken.add((pick[4], pick[1]))
        units.remove(pick)
        actions.append(("unit", *pick[1:]))
        now += unit_us
        done[pick[1:3]] += 1
        if done[pick[1:3]] == 8:
            actions.append(("finish", *pick[1:3]))
            if all(done[oz, pick[2]] == 8 for oz in range(RING)):
                actions.append(("post", pick[2]))
            now += unit_us
        return True

    while arrivals or units:
        if arrivals and arrivals[0][0] <= now:
            _, _, key = heapq.heappop(arrivals)
            now += event_us
            if key[0] == "W":
                actions.append(("swapped", key[1]))
                pieces[1, 0] += 1
                offer(1, key[1])
            elif key[0] == "G":
                actions.append(("gradients", *key[1:]))
                pieces[key[1:3]] += 1
                if key[2:] == (3, 0):
                    send("x+", ("G", key[1], 2, 0), piece_bytes)
                elif key[2:] == (1, 1):
                    send("x-", ("G", key[1], 2, 1), piece_bytes)
            else:
                actions.append(("wait", key) if any(key[1:3]) else ("own", key[0]))
                if key[3]:
                    got[key[:3]] = got.get(key[:3], 0) + 1
                    if got[key[:3]] == 2:
                        complete(key)
                else:
                    complete(key)
            compute()
            continue
        if (not arrivals or arrivals[0][0] > now + 1.5 * unit_us) and compute():
            continue
        nexts = [a[0] for a in arrivals[:1]] + [u[0] for u in units if pieces[u[2], u[3]] == 2]
        now = max(now + 1e-6, min(nexts))
    return actions, now


def kernel(actions, spans, ids, g_hbm, p_hbm, q_hbm, out_ref, gall, pin, qin, buf, acc, prods, rsq, qsq,
           fsend, frecv, lsend, lrecv, local, ws, wr, gs, gr, ts, tr, ms, mr, ds, dr, fs, fr):
    s, a = lax.axis_index("seq"), lax.axis_index("layer")
    core, z, y = s % 2, (s // 2) % ZS, s // (2 * ZS)
    feats, width = p_hbm.shape
    rows, queries = g_hbm.shape[0], q_hbm.shape[0]
    part_rows = queries // XS
    mine = y % 2 + 2 * core
    group = z % 2
    partner = s + 1 - 2 * core

    def seq(yy, zz, cc):
        return (yy * ZS + zz) * 2 + cc

    def slot(yy, jj, cc):
        return (yy * RING + jj) * 2 + cc

    swap_y, swap_core = y - y % 2 + a % 2, a // 2
    swap_to = (seq(swap_y, z, swap_core), mine)
    across = z + 1 - 2 * group
    ahead = {
        "y+": (seq((y + 1) % YS, z, core), a),
        "y-": (seq((y + YS - 1) % YS, z, core), a),
        "z+": (seq(y, (z + 2) % ZS, core), a),
        "z-": (seq(y, (z + ZS - 2) % ZS, core), a),
        "x+": (s, (a + 1) % XS),
        "x-": (s, (a + XS - 1) % XS),
    }
    targets = [(3 + k, 1, (a + k) % XS, (seq(y, across, core), (a + k) % XS)) for k in (2, 1, 3, 0)]
    targets += [(k - 1, 0, (a + k) % XS, (s, (a + k) % XS)) for k in (2, 1, 3)]
    ypos = [(y + k) % YS for k in range(YS)]
    jpos = [(z // 2 + k) % RING for k in range(RING)]

    def remote(src, dst, send, recv, to):
        return pltpu.make_async_remote_copy(
            src_ref=src, dst_ref=dst, send_sem=send, recv_sem=recv, device_id=to, device_id_type=MESH
        )

    p_in = pltpu.make_async_copy(p_hbm, pin, local.at[0])
    q_in = pltpu.make_async_copy(q_hbm, qin, local.at[1])
    g_in = pltpu.make_async_copy(g_hbm, gall.at[group, a], local.at[2])
    p_in.start()
    q_in.start()
    g_in.start()

    barrier = pltpu.get_barrier_semaphore()
    around = [*ahead.values(), *(target[3] for target in targets), (partner, a)]
    del around[4:6]
    for device in around:
        pl.semaphore_signal(barrier, inc=1, device_id=device, device_id_type=MESH)

    @pl.when(a != mine)
    def _():
        pl.semaphore_signal(barrier, inc=1, device_id=swap_to, device_id_type=MESH)
        pl.semaphore_wait(barrier, len(around) + 1)

    @pl.when(a == mine)
    def _():
        pl.semaphore_wait(barrier, len(around))

    q_rows = qin.at[pl.ds(pl.multiple_of(a * part_rows, part_rows), part_rows)]
    cuts = [span[0] for span in spans]
    last_part = len(cuts) - 1
    cuts = [*cuts[:-1], (cuts[-1][0], feats), (feats, feats + part_rows)]
    here = slot(y, z // 2, core)

    def swap(k, place):
        first, last = cuts[k]
        view = q_rows if k > last_part else pin.at[pl.ds(first, last - first)]
        return remote(view, buf.at[place, pl.ds(first, last - first)], ts.at[k], tr.at[k], swap_to)

    def stay(k):
        first, last = cuts[k]
        view = q_rows if k > last_part else pin.at[pl.ds(first, last - first)]
        return pltpu.make_async_copy(view, buf.at[here, pl.ds(first, last - first)], local.at[3 + k])

    p_in.wait()
    q_in.wait()

    @pl.when(a != mine)
    def _():
        for k in range(len(cuts)):
            swap(k, slot(swap_y, z // 2, swap_core)).start()

    @pl.when(a == mine)
    def _():
        for k in range(len(cuts)):
            stay(k).start()

    def arrived(parts):
        @pl.when(a != mine)
        def _():
            for k in parts:
                swap(k, here).wait_recv()

        @pl.when(a == mine)
        def _():
            for k in parts:
                stay(k).wait()

    piece = rows // 2

    def handed(h, whose):
        view = gall.at[whose, a, pl.ds(h * piece, piece)]
        return remote(view, view, ws.at[h], wr.at[h], (seq(y, across, core), a))

    def ringed(other, came, h, layer):
        view = gall.at[1 - group if other else group, layer, pl.ds(h * piece, piece)]
        k = other * 6 + {3: 0, 1: 2, 2: 4}[came] + h
        link = {3: "x+", 1: "x-", 2: "x-" if h else "x+"}[came]
        return remote(view, view, gs.at[k], gr.at[k], ahead[link])

    left, right, far = (a + XS - 1) % XS, (a + 1) % XS, (a + 2) % XS
    g_in.wait()
    handed(0, group).start()
    for h in range(2):
        ringed(0, 3, h, a).start()
        ringed(0, 1, h, a).start()

    def block(key):
        part, oy, oz, which = key
        first, last = spans[part][which]
        return buf.at[slot(ypos[oy], jpos[oz], core), pl.ds(first, last - first)]

    def message(link, key, view):
        return remote(view, view, ms.at[ids[key]], mr.at[ids[key]], ahead[link])

    def shared(part, oy, oz, whose):
        first, last = spans[part][0]
        view = buf.at[slot(ypos[oy], jpos[oz], whose), pl.ds(first, last - first)]
        k = (part * YS + oy) * RING + oz
        return remote(view, view, ds.at[k], dr.at[k], (partner, a))

    for ref in (acc, prods, rsq, qsq):
        ref[...] = jnp.zeros(ref.shape, jnp.float32)

    def unit(jj, rowset, layer, k):
        parity, whose = layer % 2, layer // 2
        deep = pl.ds(k * (feats // 2), feats // 2)
        right_side = jnp.concatenate([buf[slot(parity + yy, jj, whose), deep, :] for yy in (0, 2)], axis=1)
        acc[jj, rowset] += jnp.dot(gall[rowset, layer, :, deep], right_side, preferred_element_type=jnp.float32)

    def finish(jj, rowset, other):
        sketch = acc[jj, rowset].astype(jnp.bfloat16)
        wide = sketch.astype(jnp.float32)
        asked = jnp.concatenate(
            [
                jnp.concatenate(
                    [buf[slot(layer % 2 + yy, jj, layer // 2), pl.ds(feats, part_rows), :] for layer in range(XS)],
                    axis=0,
                )
                for yy in (0, 2)
            ],
            axis=1,
        )
        own = wide * wide
        rsq[other] += own[:, :width] + own[:, width:]
        if other:
            asked_wide = asked.astype(jnp.float32)
            ask = asked_wide * asked_wide
            qsq[...] += ask[:, :width] + ask[:, width:]
        prods[other] += lax.dot_general(
            sketch, asked, (((1,), (1,)), ((), ())), preferred_element_type=jnp.float32
        )

    ones = jnp.ones((8, width), jnp.float32)

    def along(squares):
        return lax.dot_general(
            ones, squares, (((1,), (1,)), ((), ())), precision=lax.Precision.HIGHEST,
            preferred_element_type=jnp.float32,
        )

    block_rows = rows // XS
    finals = []
    query_lines = []

    def post(other):
        if not query_lines:
            query_lines.append(along(qsq[...]))
        query_line = query_lines[0]
        upper = lax.broadcasted_iota(jnp.int32, query_line.shape, 0) < 4
        for layer in range(XS):
            fsend[other, layer] = prods[other, layer * block_rows : (layer + 1) * block_rows].astype(jnp.bfloat16)
        lsend[other] = jnp.where(upper, along(rsq[other]), query_line)
        for k, which, layer, device in targets:
            if which == other:
                for source, into, sem in ((fsend.at[other, layer], frecv.at[k], k), (lsend.at[other], lrecv.at[k], 7 + k)):
                    finals.append(remote(source, into, fs.at[sem], fr.at[sem], device))
                    finals[-1].start()

    used = {}
    for action in actions:
        if action[0] == "own":
            arrived((action[1],) if action[1] < last_part else (last_part, last_part + 1))
        elif action[0] == "send":
            for link, new in action[2]:
                used[new] = link
                message(link, new, block((*action[1], new[3]))).start()
            if action[1] == (0, 0, 0):
                handed(1, group).start()
        elif action[0] == "share":
            shared(*action[1:], core).start()
        elif action[0] == "wait":
            key = action[1]
            message(used[key], key, block(key)).wait_recv()
        elif action[0] == "swapped":
            h = action[1]
            handed(h, 1 - group).wait_recv()
            ringed(1, 3, h, a).start()
            ringed(1, 1, h, a).start()
        elif action[0] == "gradients":
            other, came, h = action[1:]
            ringed(other, came, h, {3: left, 1: right, 2: far}[came]).wait_recv()
            if (came, h) == (3, 0):
                ringed(other, 2, 0, left).start()
            elif (came, h) == (1, 1):
                ringed(other, 2, 1, right).start()
        elif action[0] == "take":
            for oy in range(YS):
                shared(action[1], oy, action[2], 1 - core).wait_recv()
        elif action[0] == "unit":
            oz, other, away, k = action[1:]
            unit(jpos[oz], 1 - group if other else group, (a + away) % XS, k)
        elif action[0] == "post":
            post(action[1])
        elif action[0] == "finish":
            oz, other = action[1:]
            finish(jpos[oz], 1 - group if other else group, other)

    total = prods[0, pl.ds(pl.multiple_of(a * block_rows, block_rows), block_rows)]
    line = lsend[0]
    for copy in finals:
        copy.wait_recv()
    for k in range(7):
        total = total + frecv[k].astype(jnp.float32)
        line = line + lrecv[k]
    at_row = lax.broadcasted_iota(jnp.int32, (block_rows, rows), 0) + a * block_rows
    chosen = (lax.broadcasted_iota(jnp.int32, (block_rows, rows), 1) == at_row).astype(jnp.float32)
    own_rows = lax.dot_general(
        chosen, line, (((1,), (1,)), ((), ())), precision=lax.Precision.HIGHEST,
        preferred_element_type=jnp.float32,
    )[:, 0:1]
    out_ref[...] = total * lax.rsqrt(own_rows + EPS) * lax.rsqrt(line[4:5] + EPS)

    for copy in finals:
        copy.wait_send()
    for h in range(2):
        handed(h, group).wait_send()

    def rung(k, carry):
        view = gall.at[0, 0, pl.ds(0, piece)]
        remote(view, view, gs.at[k], gr.at[k], (partner, a)).wait_send()
        return carry

    lax.fori_loop(0, 12, rung, 0)

    @pl.when(a != mine)
    def _():
        for k in range(len(cuts)):
            swap(k, slot(swap_y, z // 2, swap_core)).wait_send()

    groups = {}
    for key in ids:
        groups.setdefault((key[0], bool(key[3])), []).append(key)
    for keys in groups.values():
        first, view = ids[keys[0]], block(keys[0])

        def sent(k, carry, view=view):
            remote(view, view, ms.at[k], mr.at[k], (partner, a)).wait_send()
            return carry

        lax.fori_loop(first, first + len(keys), sent, 0)

    for part in range(len(spans)):
        first, last = spans[part][0]
        view = buf.at[0, pl.ds(first, last - first)]

        def given(k, carry, view=view):
            remote(view, view, ds.at[k], dr.at[k], (partner, a)).wait_send()
            return carry

        lax.fori_loop(part * YS * RING, (part + 1) * YS * RING, given, 0)


def shards(gradients, projection, queries):
    rows, feats = gradients.shape
    width = projection.shape[1]
    count = queries.shape[0]
    deep = feats + count // XS
    assert sum(part[1] for part in PARTS) == deep
    spans = spans_of(PARTS)
    actions, _ = plan(width * 2, rows * feats)
    keys = sorted((action[1] for action in actions if action[0] == "wait"), key=lambda k: (k[0], k[3] > 0, k))
    ids = {key: k for k, key in enumerate(keys)}
    dma = pltpu.SemaphoreType.DMA
    cuts = len(PARTS) + 1
    return pl.pallas_call(
        functools.partial(kernel, actions, spans, ids),
        out_shape=jax.ShapeDtypeStruct((rows // XS, count), jnp.float32),
        in_specs=[pl.BlockSpec(memory_space=pl.ANY)] * 3,
        out_specs=pl.BlockSpec(memory_space=pltpu.VMEM),
        scratch_shapes=[
            pltpu.VMEM((2, XS, rows, feats), jnp.bfloat16),
            pltpu.VMEM((feats, width), jnp.bfloat16),
            pltpu.VMEM((count, width), jnp.bfloat16),
            pltpu.VMEM((2 * YS * RING, deep, width), jnp.bfloat16),
            pltpu.VMEM((RING, 2, rows, 2 * width), jnp.float32),
            pltpu.VMEM((2, rows, count), jnp.float32),
            pltpu.VMEM((2, rows, width), jnp.float32),
            pltpu.VMEM((count, width), jnp.float32),
            pltpu.VMEM((2, XS, rows // XS, count), jnp.bfloat16),
            pltpu.VMEM((7, rows // XS, count), jnp.bfloat16),
            pltpu.VMEM((2, 8, count), jnp.float32),
            pltpu.VMEM((7, 8, count), jnp.float32),
            dma((3 + cuts,)), dma((2,)), dma((2,)), dma((12,)), dma((12,)), dma((cuts,)), dma((cuts,)),
            dma((len(keys),)), dma((len(keys),)), dma((len(PARTS) * YS * RING,)), dma((len(PARTS) * YS * RING,)), dma((14,)), dma((14,)),
        ],
        compiler_params=pltpu.CompilerParams(
            collective_id=0, has_side_effects=True, vmem_limit_bytes=56 * 2**20
        ),
    )(gradients, projection, queries) * math.sqrt(K)


def solution(mesh):
    placed = (P("seq", "layer"), P("layer", "seq"), P(None, "seq"))
    return jax.shard_map(
        shards, mesh=mesh, in_specs=placed, out_specs=P(("seq", "layer"), None), check_vma=False
    )
```

```python
import functools
import heapq
import math

import jax
import jax.numpy as jnp
from jax import lax
from jax.experimental import pallas as pl
from jax.experimental.pallas import tpu as pltpu
from jax.sharding import PartitionSpec as P

MESH = pl.DeviceIdType.MESH
K = 8192
EPS = 1e-06
XS, YS, ZS = 4, 4, 8
RING = ZS // 2
PARTS = (("B", 512), ("B", 576))


def spans_of(parts):
    spans, first = [], 0
    for _, rows in parts:
        mid, last = first + rows // 2, first + rows
        spans.append({0: (first, last), 1: (first, mid), 2: (mid, last)})
        first = last
    return spans


def forwards(key):
    part, oy, oz, half = key
    own_y = [("y+", (part, 3, oz, 0)), ("y-", (part, 1, oz, 0))]
    own_z = [("z+", (part, oy, 3, 0)), ("z-", (part, oy, 1, 0))]
    on_y = {0: own_y, 3: [("y+", (part, 2, oz, 1))], 1: [("y-", (part, 2, oz, 2))], 2: []}
    on_z = {0: own_z, 3: [("z+", (part, oy, 2, 1))], 1: [("z-", (part, oy, 2, 2))], 2: []}
    if PARTS[part][0] == "A":
        return on_y[oy] + own_z if oz == 0 else on_z[oz]
    return (own_y + own_z if oz == 0 else on_z[oz] + own_y) if oy == 0 else on_y[oy]


def plan(row_bytes, piece_bytes):
    lag, unit_us, event_us, start_us = 3.2, 0.08, 0.08, 4.0
    rate = {"y+": 42e3, "y-": 42e3, "z+": 21e3, "z-": 21e3, "x+": 46.6e3, "x-": 46.6e3}
    free = dict.fromkeys(rate, 0.0)
    free["x+"] = free["x-"] = 6.0
    arrivals, order, actions = [], 0, []
    mine, got = {}, {}
    pieces = {(group, away): 0 for group in range(2) for away in range(XS)}
    pieces[0, 0] = 2
    units, taken = [], set()
    now = 0.0

    def send(link, key, size):
        nonlocal order
        begin = max(now, free[link])
        free[link] = begin + size / rate[link]
        heapq.heappush(arrivals, (free[link] + lag, order, key))
        order += 1

    def at_time(when, key):
        nonlocal order
        heapq.heappush(arrivals, (when, order, key))
        order += 1

    def complete(key):
        part, oy, oz, half = key
        sent = forwards(key)
        for link, new in sent:
            send(link, new, PARTS[part][1] * row_bytes / (2 if new[3] else 1))
        actions.append(("send", key[:3], sent))
        actions.append(("share", *key[:3]))
        mine[part, oz] = mine.get((part, oz), 0) + 1
        if mine[part, oz] == YS:
            units.extend((now + 2.0, oz, group, away, part) for group in (1, 0) for away in (0, 1, 3, 2))

    def offer(group, h):
        send("x+", ("G", group, 3, h), piece_bytes)
        send("x-", ("G", group, 1, h), piece_bytes)

    at = start_us
    for part, (_, rows) in enumerate(PARTS):
        at += rows * row_bytes / 46.6e3
        at_time(at, (part, 0, 0, 0))
    offer(0, 0)
    offer(0, 1)
    at_time(10.0, ("W", 0))
    at_time(20.0, ("W", 1))
    done = {(oz, group): 0 for oz in range(RING) for group in range(2)}

    def compute():
        nonlocal now
        ready = [u for u in units if u[0] <= now and pieces[u[2], u[3]] == 2]
        if not ready:
            return False
        pick = ready[0]
        if (pick[4], pick[1]) not in taken:
            actions.append(("take", pick[4], pick[1]))
            taken.add((pick[4], pick[1]))
        units.remove(pick)
        actions.append(("unit", *pick[1:]))
        now += unit_us
        done[pick[1:3]] += 1
        if done[pick[1:3]] == 8:
            actions.append(("finish", *pick[1:3]))
            if all(done[oz, pick[2]] == 8 for oz in range(RING)):
                actions.append(("post", pick[2]))
            now += unit_us
        return True

    while arrivals or units:
        if arrivals and arrivals[0][0] <= now:
            _, _, key = heapq.heappop(arrivals)
            now += event_us
            if key[0] == "W":
                actions.append(("swapped", key[1]))
                pieces[1, 0] += 1
                offer(1, key[1])
            elif key[0] == "G":
                actions.append(("gradients", *key[1:]))
                pieces[key[1:3]] += 1
                if key[2:] == (3, 0):
                    send("x+", ("G", key[1], 2, 0), piece_bytes)
                elif key[2:] == (1, 1):
                    send("x-", ("G", key[1], 2, 1), piece_bytes)
            else:
                actions.append(("wait", key) if any(key[1:3]) else ("own", key[0]))
                if key[3]:
                    got[key[:3]] = got.get(key[:3], 0) + 1
                    if got[key[:3]] == 2:
                        complete(key)
                else:
                    complete(key)
            compute()
            continue
        if (not arrivals or arrivals[0][0] > now + 1.5 * unit_us) and compute():
            continue
        nexts = [a[0] for a in arrivals[:1]] + [u[0] for u in units if pieces[u[2], u[3]] == 2]
        now = max(now + 1e-6, min(nexts))
    return actions, now


def kernel(actions, spans, ids, g_hbm, p_hbm, q_hbm, out_ref, gall, pin, qin, buf, acc, prods, rsq, qsq,
           fsend, frecv, lsend, lrecv, local, ws, wr, gs, gr, ts, tr, ms, mr, ds, dr, fs, fr):
    s, a = lax.axis_index("seq"), lax.axis_index("layer")
    core, z, y = s % 2, (s // 2) % ZS, s // (2 * ZS)
    feats, width = p_hbm.shape
    rows, queries = g_hbm.shape[0], q_hbm.shape[0]
    part_rows = queries // XS
    mine = y % 2 + 2 * core
    group = z % 2
    partner = s + 1 - 2 * core

    def seq(yy, zz, cc):
        return (yy * ZS + zz) * 2 + cc

    def slot(yy, jj, cc):
        return (yy * RING + jj) * 2 + cc

    swap_y, swap_core = y - y % 2 + a % 2, a // 2
    swap_to = (seq(swap_y, z, swap_core), mine)
    across = z + 1 - 2 * group
    ahead = {
        "y+": (seq((y + 1) % YS, z, core), a),
        "y-": (seq((y + YS - 1) % YS, z, core), a),
        "z+": (seq(y, (z + 2) % ZS, core), a),
        "z-": (seq(y, (z + ZS - 2) % ZS, core), a),
        "x+": (s, (a + 1) % XS),
        "x-": (s, (a + XS - 1) % XS),
    }
    targets = [(3 + k, 1, (a + k) % XS, (seq(y, across, core), (a + k) % XS)) for k in (2, 1, 3, 0)]
    targets += [(k - 1, 0, (a + k) % XS, (s, (a + k) % XS)) for k in (2, 1, 3)]
    ypos = [(y + k) % YS for k in range(YS)]
    jpos = [(z // 2 + k) % RING for k in range(RING)]

    def remote(src, dst, send, recv, to):
        return pltpu.make_async_remote_copy(
            src_ref=src, dst_ref=dst, send_sem=send, recv_sem=recv, device_id=to, device_id_type=MESH
        )

    p_in = pltpu.make_async_copy(p_hbm, pin, local.at[0])
    q_in = pltpu.make_async_copy(q_hbm, qin, local.at[1])
    g_in = pltpu.make_async_copy(g_hbm, gall.at[group, a], local.at[2])
    p_in.start()
    q_in.start()
    g_in.start()

    barrier = pltpu.get_barrier_semaphore()
    around = [*ahead.values(), *(target[3] for target in targets), (partner, a)]
    del around[4:6]
    for device in around:
        pl.semaphore_signal(barrier, inc=1, device_id=device, device_id_type=MESH)

    @pl.when(a != mine)
    def _():
        pl.semaphore_signal(barrier, inc=1, device_id=swap_to, device_id_type=MESH)
        pl.semaphore_wait(barrier, len(around) + 1)

    @pl.when(a == mine)
    def _():
        pl.semaphore_wait(barrier, len(around))

    q_rows = qin.at[pl.ds(pl.multiple_of(a * part_rows, part_rows), part_rows)]
    cuts = [span[0] for span in spans]
    last_part = len(cuts) - 1
    cuts = [*cuts[:-1], (cuts[-1][0], feats), (feats, feats + part_rows)]
    here = slot(y, z // 2, core)

    def swap(k, place):
        first, last = cuts[k]
        view = q_rows if k > last_part else pin.at[pl.ds(first, last - first)]
        return remote(view, buf.at[place, pl.ds(first, last - first)], ts.at[k], tr.at[k], swap_to)

    def stay(k):
        first, last = cuts[k]
        view = q_rows if k > last_part else pin.at[pl.ds(first, last - first)]
        return pltpu.make_async_copy(view, buf.at[here, pl.ds(first, last - first)], local.at[3 + k])

    p_in.wait()
    q_in.wait()

    @pl.when(a != mine)
    def _():
        for k in range(len(cuts)):
            swap(k, slot(swap_y, z // 2, swap_core)).start()

    @pl.when(a == mine)
    def _():
        for k in range(len(cuts)):
            stay(k).start()

    def arrived(parts):
        @pl.when(a != mine)
        def _():
            for k in parts:
                swap(k, here).wait_recv()

        @pl.when(a == mine)
        def _():
            for k in parts:
                stay(k).wait()

    piece = rows // 2

    def handed(h, whose):
        view = gall.at[whose, a, pl.ds(h * piece, piece)]
        return remote(view, view, ws.at[h], wr.at[h], (seq(y, across, core), a))

    def ringed(other, came, h, layer):
        view = gall.at[1 - group if other else group, layer, pl.ds(h * piece, piece)]
        k = other * 6 + {3: 0, 1: 2, 2: 4}[came] + h
        link = {3: "x+", 1: "x-", 2: "x-" if h else "x+"}[came]
        return remote(view, view, gs.at[k], gr.at[k], ahead[link])

    left, right, far = (a + XS - 1) % XS, (a + 1) % XS, (a + 2) % XS
    g_in.wait()
    handed(0, group).start()
    for h in range(2):
        ringed(0, 3, h, a).start()
        ringed(0, 1, h, a).start()

    def block(key):
        part, oy, oz, which = key
        first, last = spans[part][which]
        return buf.at[slot(ypos[oy], jpos[oz], core), pl.ds(first, last - first)]

    def message(link, key, view):
        return remote(view, view, ms.at[ids[key]], mr.at[ids[key]], ahead[link])

    def shared(part, oy, oz, whose):
        first, last = spans[part][0]
        view = buf.at[slot(ypos[oy], jpos[oz], whose), pl.ds(first, last - first)]
        k = (part * YS + oy) * RING + oz
        return remote(view, view, ds.at[k], dr.at[k], (partner, a))

    for ref in (acc, prods, rsq, qsq):
        ref[...] = jnp.zeros(ref.shape, jnp.float32)

    def unit(jj, rowset, layer, k):
        parity, whose = layer % 2, layer // 2
        deep = pl.ds(k * (feats // 2), feats // 2)
        right_side = jnp.concatenate([buf[slot(parity + yy, jj, whose), deep, :] for yy in (0, 2)], axis=1)
        acc[jj, rowset] += jnp.dot(gall[rowset, layer, :, deep], right_side, preferred_element_type=jnp.float32)

    def finish(jj, rowset, other):
        sketch = acc[jj, rowset].astype(jnp.bfloat16)
        wide = sketch.astype(jnp.float32)
        asked = jnp.concatenate(
            [
                jnp.concatenate(
                    [buf[slot(layer % 2 + yy, jj, layer // 2), pl.ds(feats, part_rows), :] for layer in range(XS)],
                    axis=0,
                )
                for yy in (0, 2)
            ],
            axis=1,
        )
        own = wide * wide
        rsq[other] += own[:, :width] + own[:, width:]
        if other:
            asked_wide = asked.astype(jnp.float32)
            ask = asked_wide * asked_wide
            qsq[...] += ask[:, :width] + ask[:, width:]
        prods[other] += lax.dot_general(
            sketch, asked, (((1,), (1,)), ((), ())), preferred_element_type=jnp.float32
        )

    ones = jnp.ones((8, width), jnp.float32)

    def along(squares):
        return lax.dot_general(
            ones, squares, (((1,), (1,)), ((), ())), precision=lax.Precision.HIGHEST,
            preferred_element_type=jnp.float32,
        )

    block_rows = rows // XS
    finals = []
    query_lines = []

    def post(other):
        if not query_lines:
            query_lines.append(along(qsq[...]))
        query_line = query_lines[0]
        row_line = along(rsq[other])
        place = lax.broadcasted_iota(jnp.int32, (8, width), 0)
        for layer in range(XS):
            fsend[other, layer] = prods[other, layer * block_rows : (layer + 1) * block_rows].astype(jnp.bfloat16)
        row_half = jnp.where(place < 2, row_line[:, :width], row_line[:, width:])
        query_half = jnp.where(place < 6, query_line[:, :width], query_line[:, width:])
        lsend[other] = jnp.where(place < 4, row_half, query_half)
        for k, which, layer, device in targets:
            if which == other:
                for source, into, sem in ((fsend.at[other, layer], frecv.at[k], k), (lsend.at[other], lrecv.at[k], 7 + k)):
                    finals.append(remote(source, into, fs.at[sem], fr.at[sem], device))
                    finals[-1].start()

    used = {}
    for action in actions:
        if action[0] == "own":
            arrived((action[1],) if action[1] < last_part else (last_part, last_part + 1))
        elif action[0] == "send":
            for link, new in action[2]:
                used[new] = link
                message(link, new, block((*action[1], new[3]))).start()
            if action[1] == (0, 0, 0):
                handed(1, group).start()
        elif action[0] == "share":
            shared(*action[1:], core).start()
        elif action[0] == "wait":
            key = action[1]
            message(used[key], key, block(key)).wait_recv()
        elif action[0] == "swapped":
            h = action[1]
            handed(h, 1 - group).wait_recv()
            ringed(1, 3, h, a).start()
            ringed(1, 1, h, a).start()
        elif action[0] == "gradients":
            other, came, h = action[1:]
            ringed(other, came, h, {3: left, 1: right, 2: far}[came]).wait_recv()
            if (came, h) == (3, 0):
                ringed(other, 2, 0, left).start()
            elif (came, h) == (1, 1):
                ringed(other, 2, 1, right).start()
        elif action[0] == "take":
            for oy in range(YS):
                shared(action[1], oy, action[2], 1 - core).wait_recv()
        elif action[0] == "unit":
            oz, other, away, k = action[1:]
            unit(jpos[oz], 1 - group if other else group, (a + away) % XS, k)
        elif action[0] == "post":
            post(action[1])
        elif action[0] == "finish":
            oz, other = action[1:]
            finish(jpos[oz], 1 - group if other else group, other)

    total = prods[0, pl.ds(pl.multiple_of(a * block_rows, block_rows), block_rows)]
    line = lsend[0]
    for copy in finals:
        copy.wait_recv()
    for k in range(7):
        total = total + frecv[k].astype(jnp.float32)
        line = line + lrecv[k]
    row_squares = jnp.concatenate(
        [jnp.broadcast_to(line[k : k + 1], line.shape) for k in (0, 2)], axis=1
    )
    query_squares = jnp.concatenate([line[4:5], line[6:7]], axis=1)
    at_row = lax.broadcasted_iota(jnp.int32, (block_rows, rows), 0) + a * block_rows
    chosen = (lax.broadcasted_iota(jnp.int32, (block_rows, rows), 1) == at_row).astype(jnp.float32)
    own_rows = lax.dot_general(
        chosen, row_squares, (((1,), (1,)), ((), ())), precision=lax.Precision.HIGHEST,
        preferred_element_type=jnp.float32,
    )[:, 0:1]
    out_ref[...] = total * lax.rsqrt(own_rows + EPS) * lax.rsqrt(query_squares + EPS)

    for copy in finals:
        copy.wait_send()
    for h in range(2):
        handed(h, group).wait_send()

    def rung(k, carry):
        view = gall.at[0, 0, pl.ds(0, piece)]
        remote(view, view, gs.at[k], gr.at[k], (partner, a)).wait_send()
        return carry

    lax.fori_loop(0, 12, rung, 0)

    @pl.when(a != mine)
    def _():
        for k in range(len(cuts)):
            swap(k, slot(swap_y, z // 2, swap_core)).wait_send()

    groups = {}
    for key in ids:
        groups.setdefault((key[0], bool(key[3])), []).append(key)
    for keys in groups.values():
        first, view = ids[keys[0]], block(keys[0])

        def sent(k, carry, view=view):
            remote(view, view, ms.at[k], mr.at[k], (partner, a)).wait_send()
            return carry

        lax.fori_loop(first, first + len(keys), sent, 0)

    for part in range(len(spans)):
        first, last = spans[part][0]
        view = buf.at[0, pl.ds(first, last - first)]

        def given(k, carry, view=view):
            remote(view, view, ds.at[k], dr.at[k], (partner, a)).wait_send()
            return carry

        lax.fori_loop(part * YS * RING, (part + 1) * YS * RING, given, 0)


def shards(gradients, projection, queries):
    rows, feats = gradients.shape
    width = projection.shape[1]
    count = queries.shape[0]
    deep = feats + count // XS
    assert sum(part[1] for part in PARTS) == deep
    spans = spans_of(PARTS)
    actions, _ = plan(width * 2, rows * feats)
    keys = sorted((action[1] for action in actions if action[0] == "wait"), key=lambda k: (k[0], k[3] > 0, k))
    ids = {key: k for k, key in enumerate(keys)}
    dma = pltpu.SemaphoreType.DMA
    cuts = len(PARTS) + 1
    return pl.pallas_call(
        functools.partial(kernel, actions, spans, ids),
        out_shape=jax.ShapeDtypeStruct((rows // XS, count), jnp.float32),
        in_specs=[pl.BlockSpec(memory_space=pl.ANY)] * 3,
        out_specs=pl.BlockSpec(memory_space=pltpu.VMEM),
        scratch_shapes=[
            pltpu.VMEM((2, XS, rows, feats), jnp.bfloat16),
            pltpu.VMEM((feats, width), jnp.bfloat16),
            pltpu.VMEM((count, width), jnp.bfloat16),
            pltpu.VMEM((2 * YS * RING, deep, width), jnp.bfloat16),
            pltpu.VMEM((RING, 2, rows, 2 * width), jnp.float32),
            pltpu.VMEM((2, rows, count), jnp.float32),
            pltpu.VMEM((2, rows, width), jnp.float32),
            pltpu.VMEM((count, width), jnp.float32),
            pltpu.VMEM((2, XS, rows // XS, count), jnp.bfloat16),
            pltpu.VMEM((7, rows // XS, count), jnp.bfloat16),
            pltpu.VMEM((2, 8, width), jnp.float32),
            pltpu.VMEM((7, 8, width), jnp.float32),
            dma((3 + cuts,)), dma((2,)), dma((2,)), dma((12,)), dma((12,)), dma((cuts,)), dma((cuts,)),
            dma((len(keys),)), dma((len(keys),)), dma((len(PARTS) * YS * RING,)), dma((len(PARTS) * YS * RING,)), dma((14,)), dma((14,)),
        ],
        compiler_params=pltpu.CompilerParams(
            collective_id=0, has_side_effects=True, vmem_limit_bytes=56 * 2**20
        ),
    )(gradients, projection, queries) * math.sqrt(K)


def solution(mesh):
    placed = (P("seq", "layer"), P("layer", "seq"), P(None, "seq"))
    return jax.shard_map(
        shards, mesh=mesh, in_specs=placed, out_specs=P(("seq", "layer"), None), check_vma=False
    )
```
